32 devices in a mesh: rep: 16 (over z, y, x), dom: 2 (over core).
Axes of the slice: x: 2, y: 2, z: 4, core: 2. Of those that a mesh axis runs over, the one named last changes fastest.
Arguments:
- protein_pos: float32 [3, 65536], P(None, ('rep', 'dom')), parts along dimension 1, may hold values from -4 to 4, as said below
- protein_vel: float32 [3, 65536], P(None, ('rep', 'dom')), parts along dimension 1, may hold values from -3 to 3
- inv_mass: float32 [65536], P(('rep', 'dom')), parts along dimension 0, may hold values from 0.0625 to 1
- bond_atoms: int32 [2, 40960], P(None, ('rep', 'dom')), parts along dimension 1, may hold values from 0 to 2047, as said below
- left_atoms: int32 [12288], P(('rep', 'dom')), parts along dimension 0, may hold values from 0 to 2047, as said below
- right_atoms: int32 [12288], P(('rep', 'dom')), parts along dimension 0, may hold values from 0 to 2047, as said below
- water_pos: float32 [9, 32768], P(None, ('rep', 'dom')), parts along dimension 1, may hold values from -3.2 to 3.2, as said below
- water_vel: float32 [9, 32768], P(None, ('rep', 'dom')), parts along dimension 1, may hold values from -3 to 3
Outputs:
- protein_velocity: float32 [3, 65536], P(None, ('rep', 'dom')), parts along dimension 1
- water_velocity: float32 [9, 32768], P(None, ('rep', 'dom')), parts along dimension 1
The draws below stay inside these ranges and needn't reach their ends.
There are 16 independent parts, one for each index of `rep`. The reference program is written for one: setup_inputs(seed, part) draws one part's arguments, and reference() takes and returns one part's arrays. A program takes and returns all parts, laid end to end along the dimension named above; each array names one. Nothing has to cross between parts.
Inputs may be any that keep to these rules, and one draw needn't show every extreme that they name: `bond_atoms`: indices within the domain's block of 2048 atoms; each column joins two different atoms; together with the cross bonds the bonds form a forest. `left_atoms`: distinct indices within the domain's block, none of them in right_atoms. `right_atoms`: distinct indices within the domain's block. `protein_pos`: every bond and every cross bond joins atoms 0.1 to 0.15 apart. `water_pos`: each column holds one rigid water: oxygen, then two hydrogens, 0.09572 from the oxygen and 0.15139 from each other.
All inputs are finite; a program needn't handle non-finite values.
Results may differ from the reference program's by a relative error of at most 0.0003.
Values sent between devices are 32-bit elements; how exact they have to be, the bound alone decides.
A program may use at most 64 MiB of HBM per device.

```python
import math
import jax
import jax.numpy as jnp
from jax import lax

PROT_DEV = 2048
HALO = 384
ORDER = 4
ITER = 2
BOND_DEV = 1280
PROTEIN = 4096
BONDS = 2560
CROSS = 768
WATERS = 2048
N_DOM = 2


oxygen_hydrogen = 0.09572


hydrogen_pair = 0.15139


def topology(key):
    base = jax.random.fold_in(key, 7)
    perms = jax.vmap(lambda single: jax.random.permutation(single, PROT_DEV))(jax.random.split(base, N_DOM)).astype(jnp.int32)
    mains = BOND_DEV - HALO
    nodes = jnp.arange(mains + 1, dtype=jnp.int32)
    parents = jnp.broadcast_to(jnp.maximum(nodes - 1, 0) // 3, (N_DOM, mains + 1)).astype(jnp.int32)
    return (perms, parents)


def draw_bond_atoms(key, part):
    perms, parents = topology(key)
    mains = BOND_DEV - HALO
    nodes = jnp.arange(1, mains + 1, dtype=jnp.int32)
    child_main = perms[:, HALO + 1:HALO + 1 + mains]
    parent_main = jnp.take_along_axis(perms, parents[:, nodes] + HALO, axis=1)
    child_cap = perms[:, HALO + mains + 1:HALO + mains + 1 + HALO]
    parent_cap = perms[:, :HALO]
    child = jnp.concatenate([child_main, child_cap], axis=1)
    parent = jnp.concatenate([parent_main, parent_cap], axis=1)
    return jnp.stack([child, parent]).reshape(2, N_DOM * BOND_DEV).astype(jnp.int32)


def draw_left_atoms(key, part):
    perms, parents = topology(key)
    return perms[:, :HALO].reshape(N_DOM * HALO).astype(jnp.int32)


def draw_right_atoms(key, part):
    perms, parents = topology(key)
    mains = BOND_DEV - HALO
    return perms[:, mains + 1:mains + 1 + HALO].reshape(N_DOM * HALO).astype(jnp.int32)


def bond_lengths(key, shape):
    return jnp.exp(jax.random.uniform(key, shape, jnp.float32, math.log(0.1), math.log(0.15)))


def random_steps(key, shape):
    keys = jax.random.split(key, 3)
    cosine = jax.random.uniform(keys[0], shape, jnp.float32, -1.0, 1.0)
    angle = jax.random.uniform(keys[1], shape, jnp.float32, 0.0, 2.0 * math.pi)
    sine = jnp.sqrt(jnp.maximum(1.0 - cosine * cosine, 0.0))
    lengths = bond_lengths(keys[2], shape)
    return jnp.stack([sine * jnp.cos(angle), sine * jnp.sin(angle), cosine], axis=1) * lengths[:, None, :]


def tetra_steps(key, index, sign):
    keys = jax.random.split(key, 2)
    table = jnp.array([[1.0, 1.0, 1.0], [1.0, -1.0, -1.0], [-1.0, 1.0, -1.0], [-1.0, -1.0, 1.0]], jnp.float32) / math.sqrt(3.0)
    pick = (index[..., None] == jnp.arange(4, dtype=jnp.int32)).astype(jnp.float32)
    direction = jnp.einsum('dnk,kc->dcn', pick, table) * sign[:, None, :]
    jitter = jnp.clip(jax.random.normal(keys[0], direction.shape, jnp.float32), -2.0, 2.0)
    direction = direction + 0.15 * jitter
    direction = direction / jnp.sqrt(jnp.sum(direction * direction, axis=1, keepdims=True))
    return direction * bond_lengths(keys[1], index.shape)[:, None, :]


def draw_protein_pos(key, part):
    perms, parents = topology(key)
    keys = jax.random.split(jax.random.fold_in(key, 21), 9)
    mains = BOND_DEV - HALO
    nodes = jnp.arange(mains + 1, dtype=jnp.int32)
    turns = jax.random.randint(keys[5], (N_DOM, mains + 1), 0, 3, dtype=jnp.int32)
    first_dir = jax.random.randint(keys[6], (N_DOM, 1), 0, 4, dtype=jnp.int32)
    slot = jnp.maximum(nodes - 1, 0) % 3
    index = jnp.broadcast_to(first_dir, (N_DOM, mains + 1)).astype(jnp.int32)
    depth = jnp.zeros((N_DOM, mains + 1), jnp.int32)
    for rounds in range(16):
        up_index = jnp.take_along_axis(index, parents, axis=1)
        up_turn = jnp.take_along_axis(turns, parents, axis=1)
        up_depth = jnp.take_along_axis(depth, parents, axis=1)
        index = jnp.where(nodes == 0, first_dir, (up_index + 1 + (slot + up_turn) % 3) % 4).astype(jnp.int32)
        depth = jnp.where(nodes == 0, 0, up_depth + 1).astype(jnp.int32)
    sign = jnp.where(depth % 2 == 1, 1.0, -1.0).astype(jnp.float32)
    steps = tetra_steps(keys[0], index, sign)
    steps = steps.at[:, :, 0].set(0.0)
    root = jax.random.uniform(keys[1], (N_DOM, 3), jnp.float32, -1.0, 1.0)
    total = steps
    pointer = parents
    for rounds in range(6):
        total = total + jnp.take_along_axis(total, jnp.broadcast_to(pointer[:, None, :], total.shape), axis=2)
        pointer = jnp.take_along_axis(pointer, pointer, axis=1)
    main_pos = total + root[:, :, None]
    anchor_pos = main_pos[:, :, mains + 1 - HALO:mains + 1]
    anchor_index = jnp.roll(index[:, mains + 1 - HALO:mains + 1], 1, axis=0)
    anchor_depth = jnp.roll(depth[:, mains + 1 - HALO:mains + 1], 1, axis=0)
    anchor_sign = jnp.where(anchor_depth % 2 == 0, 1.0, -1.0).astype(jnp.float32)
    cap_index = (anchor_index + 1 + jax.random.randint(keys[7], (N_DOM, HALO), 0, 3, dtype=jnp.int32)) % 4
    child_index = (cap_index + 1 + jax.random.randint(keys[8], (N_DOM, HALO), 0, 3, dtype=jnp.int32)) % 4
    cap_pos = jnp.roll(anchor_pos, 1, axis=0) + tetra_steps(keys[2], cap_index, anchor_sign)
    child_pos = cap_pos + tetra_steps(keys[3], child_index, -anchor_sign)
    lone_pos = root[:, :, None] + random_steps(keys[4], (N_DOM, HALO - 1))

    def place(perm, main_part, cap_part, child_part, lone_part):
        field = jnp.zeros((3, PROT_DEV), jnp.float32)
        field = field.at[:, perm[HALO:HALO + mains + 1]].set(main_part)
        field = field.at[:, perm[:HALO]].set(cap_part)
        field = field.at[:, perm[HALO + mains + 1:HALO + mains + 1 + HALO]].set(child_part)
        return field.at[:, perm[PROT_DEV - HALO + 1:]].set(lone_part)
    placed = jax.vmap(place)(perms, main_pos, cap_pos, child_pos, lone_pos)
    return jnp.transpose(placed, (1, 0, 2)).reshape(3, N_DOM * PROT_DEV)


def draw_water_pos(key, part):
    keys = jax.random.split(jax.random.fold_in(key, 31), 4)
    oxygen = jax.random.uniform(keys[0], (3, WATERS), jnp.float32, -3.0, 3.0)
    first_angle = jax.random.uniform(keys[1], (WATERS,), jnp.float32, -math.pi, math.pi)
    second_angle = jax.random.uniform(keys[2], (WATERS,), jnp.float32, -math.pi, math.pi)
    third_angle = jax.random.uniform(keys[3], (WATERS,), jnp.float32, -math.pi, math.pi)
    cos_a, sin_a = (jnp.cos(first_angle), jnp.sin(first_angle))
    cos_b, sin_b = (jnp.cos(second_angle), jnp.sin(second_angle))
    cos_c, sin_c = (jnp.cos(third_angle), jnp.sin(third_angle))
    column_one = jnp.stack([cos_a * cos_c - sin_a * cos_b * sin_c, sin_a * cos_c + cos_a * cos_b * sin_c, sin_b * sin_c])
    column_two = jnp.stack([-cos_a * sin_c - sin_a * cos_b * cos_c, -sin_a * sin_c + cos_a * cos_b * cos_c, sin_b * cos_c])
    half = 0.5 * hydrogen_pair
    height = math.sqrt(oxygen_hydrogen * oxygen_hydrogen - half * half)
    first = oxygen + half * column_one - height * column_two
    second = oxygen - half * column_one - height * column_two
    return jnp.concatenate([oxygen, first, second], axis=0)


def block_levels(own_key, shape, shards, least, high):
    gain = 1.0
    for axis_at, shards_of in shards:
        draws = jax.random.uniform(jax.random.fold_in(jax.random.fold_in(own_key, 6), axis_at), (shards_of,), jnp.float32, least / len(shards), high / len(shards))
        gain = gain * jnp.repeat(jnp.exp(draws), shape[axis_at] // shards_of).reshape((-1,) + (1,) * (len(shape) - 1 - axis_at))
    return gain


def gaussian(key, dims, spread, bound, cuts=(), kind=jnp.bfloat16):
    level = block_levels(key, dims, cuts, -0.22, 0.18) if cuts else 1.0
    entries = jax.random.normal(key, dims, jnp.float32) * spread * level
    return jnp.minimum(jnp.maximum(entries, -bound), bound).astype(kind)


def setup_inputs(seed: int = 0, part: int = 0) -> dict:
    seeds = jax.random.split(jax.random.key(seed), 9)
    part_splits = jax.random.split(jax.random.fold_in(seeds[8], part), 9)
    return {
        "protein_pos": draw_protein_pos(jax.random.fold_in(jax.random.fold_in(seeds[8], part), 71), part),
        "protein_vel": gaussian(part_splits[1], (3, PROTEIN), 1.0, 3.0, ((1, 2),), jnp.float32),
        "inv_mass": jnp.clip(jnp.exp(math.log(1.0) - 2.7725887 * jax.random.uniform(part_splits[2], (PROTEIN,), jnp.float32) ** block_levels(part_splits[2], (PROTEIN,), ((0, 2),), -0.2, 0.2)), 0.0625, 1.0),
        "bond_atoms": draw_bond_atoms(jax.random.fold_in(jax.random.fold_in(seeds[8], part), 71), part),
        "left_atoms": draw_left_atoms(jax.random.fold_in(jax.random.fold_in(seeds[8], part), 71), part),
        "right_atoms": draw_right_atoms(jax.random.fold_in(jax.random.fold_in(seeds[8], part), 71), part),
        "water_pos": draw_water_pos(jax.random.fold_in(jax.random.fold_in(seeds[8], part), 71), part),
        "water_vel": gaussian(part_splits[7], (9, WATERS), 1.0, 3.0, ((1, 2),), jnp.float32),
    }


time_step = 0.002
mass_oxygen = 15.9994
mass_hydrogen = 1.008
oxygen_hydrogen = 0.09572
hydrogen_pair = 0.15139
total_mass = mass_oxygen + 2.0 * mass_hydrogen
half_pair = 0.5 * hydrogen_pair
water_height = math.sqrt(oxygen_hydrogen * oxygen_hydrogen - half_pair * half_pair)
oxygen_reach = 2.0 * mass_hydrogen * water_height / total_mass
hydrogen_reach = water_height - oxygen_reach

def cross_product(left, right):
    return jnp.stack([left[1] * right[2] - left[2] * right[1], left[2] * right[0] - left[0] * right[2], left[0] * right[1] - left[1] * right[0]])

def inner(left, right):
    return lax.optimization_barrier(jnp.sum(left * right, axis=0))

def settle(before, after):
    old_oxygen, old_first, old_second = (before[0:3], before[3:6], before[6:9])
    new_oxygen, new_first, new_second = (after[0:3], after[3:6], after[6:9])
    center = (mass_oxygen * new_oxygen + mass_hydrogen * (new_first + new_second)) / total_mass
    old_b = old_first - old_oxygen
    old_c = old_second - old_oxygen
    rel_a = new_oxygen - center
    rel_b = new_first - center
    rel_c = new_second - center
    normal = cross_product(old_b, old_c)
    side = cross_product(rel_a, normal)
    upward = cross_product(normal, side)
    axis_z = normal / jnp.sqrt(inner(normal, normal))
    axis_x = side / jnp.sqrt(inner(side, side))
    axis_y = upward / jnp.sqrt(inner(upward, upward))
    oldb_x = inner(axis_x, old_b)
    oldb_y = inner(axis_y, old_b)
    oldc_x = inner(axis_x, old_c)
    oldc_y = inner(axis_y, old_c)
    newa_z = inner(axis_z, rel_a)
    newb_x = inner(axis_x, rel_b)
    newb_y = inner(axis_y, rel_b)
    newb_z = inner(axis_z, rel_b)
    newc_x = inner(axis_x, rel_c)
    newc_y = inner(axis_y, rel_c)
    newc_z = inner(axis_z, rel_c)
    sin_phi = newa_z / oxygen_reach
    cos_phi = jnp.sqrt(1.0 - sin_phi * sin_phi)
    sin_psi = (newb_z - newc_z) / (2.0 * half_pair * cos_phi)
    cos_psi = jnp.sqrt(1.0 - sin_psi * sin_psi)
    rest_ay = oxygen_reach * cos_phi
    rest_bx = -half_pair * cos_psi
    lowered = -hydrogen_reach * cos_phi
    tilted = half_pair * sin_psi * sin_phi
    rest_by = lowered - tilted
    rest_cy = lowered + tilted
    alpha = rest_bx * (oldb_x - oldc_x) + oldb_y * rest_by + oldc_y * rest_cy
    beta = rest_bx * (oldc_y - oldb_y) + oldb_x * rest_by + oldc_x * rest_cy
    gamma = oldb_x * newb_y - newb_x * oldb_y + oldc_x * newc_y - newc_x * oldc_y
    summed = alpha * alpha + beta * beta
    sin_theta = (alpha * gamma - beta * jnp.sqrt(summed - gamma * gamma)) / summed
    cos_theta = jnp.sqrt(1.0 - sin_theta * sin_theta)
    final_ax = -rest_ay * sin_theta
    final_ay = rest_ay * cos_theta
    final_bx = rest_bx * cos_theta - rest_by * sin_theta
    final_by = rest_bx * sin_theta + rest_by * cos_theta
    final_cx = -rest_bx * cos_theta - rest_cy * sin_theta
    final_cy = -rest_bx * sin_theta + rest_cy * cos_theta
    oxygen = center + axis_x * final_ax + axis_y * final_ay + axis_z * newa_z
    first = center + axis_x * final_bx + axis_y * final_by + axis_z * newb_z
    second = center + axis_x * final_cx + axis_y * final_cy + axis_z * newc_z
    return jnp.concatenate([oxygen, first, second], axis=0)

def reference(protein_pos, protein_vel, inv_mass, bond_atoms, left_atoms, right_atoms, water_pos, water_vel):
    bond_domain = jnp.arange(BONDS, dtype=jnp.int32) // BOND_DEV
    slot_domain = jnp.arange(CROSS, dtype=jnp.int32) // HALO
    next_domain = (slot_domain + 1) % N_DOM
    anchors = right_atoms + slot_domain * PROT_DEV
    capped = jnp.roll(left_atoms, -HALO) + next_domain * PROT_DEV
    first = jnp.concatenate([bond_atoms[0] + bond_domain * PROT_DEV, anchors]).astype(jnp.int32)
    second = jnp.concatenate([bond_atoms[1] + bond_domain * PROT_DEV, capped]).astype(jnp.int32)
    moved = protein_pos + time_step * protein_vel
    diff = protein_pos[:, first] - protein_pos[:, second]
    length = jnp.sqrt(inner(diff, diff))
    unit = diff / length
    scale = 1.0 / jnp.sqrt(inv_mass[first] + inv_mass[second])

    def atom_field(values):
        weighted = unit * (scale * values)
        force = jnp.zeros((3, PROTEIN), jnp.float32).at[:, first].add(weighted).at[:, second].add(-weighted)
        return inv_mass * force

    def expand(rhs):
        total = rhs
        current = rhs
        for order_index in range(ORDER):
            field = atom_field(current)
            current = current - scale * inner(unit, field[:, first] - field[:, second])
            total = total + current
        return total
    rhs = scale * (inner(unit, moved[:, first] - moved[:, second]) - length)
    delta = -atom_field(expand(rhs))
    for round_index in range(ITER):
        now = moved + delta
        gap = now[:, first] - now[:, second]
        target = jnp.sqrt(2.0 * length * length - inner(gap, gap))
        rhs = scale * (length - target)
        delta = delta - atom_field(expand(rhs))
    protein_velocity = protein_vel + delta / time_step
    water_moved = water_pos + time_step * water_vel
    settled = settle(water_pos, water_moved)
    water_velocity = water_vel + (settled - water_moved) / time_step
    return (protein_velocity, water_velocity)
```

```python
import functools
import math

import jax
import jax.numpy as jnp
from jax import lax
from jax.experimental import pallas as pl
from jax.experimental.pallas import tpu as pltpu
from jax.sharding import PartitionSpec as P

ORDER = 4
ITER = 2
LANES = 128
SUB = 8
WIDE = 2 * LANES
F8 = jnp.float8_e4m3fn


time_step = 0.002
mass_oxygen = 15.9994
mass_hydrogen = 1.008
oxygen_hydrogen = 0.09572
hydrogen_pair = 0.15139
total_mass = mass_oxygen + 2.0 * mass_hydrogen
half_pair = 0.5 * hydrogen_pair
water_height = math.sqrt(oxygen_hydrogen * oxygen_hydrogen - half_pair * half_pair)
oxygen_reach = 2.0 * mass_hydrogen * water_height / total_mass
hydrogen_reach = water_height - oxygen_reach


def cross_product(left, right):
    return [
        left[1] * right[2] - left[2] * right[1],
        left[2] * right[0] - left[0] * right[2],
        left[0] * right[1] - left[1] * right[0],
    ]


def inner(left, right):
    return left[0] * right[0] + left[1] * right[1] + left[2] * right[2]


def minus(left, right):
    return [a - b for a, b in zip(left, right)]


def settle(before, after):
    old_oxygen, old_first, old_second = (before[0:3], before[3:6], before[6:9])
    new_oxygen, new_first, new_second = (after[0:3], after[3:6], after[6:9])
    center = [
        (mass_oxygen * o + mass_hydrogen * (f + s)) / total_mass
        for o, f, s in zip(new_oxygen, new_first, new_second)
    ]
    old_b = minus(old_first, old_oxygen)
    old_c = minus(old_second, old_oxygen)
    rel_a = minus(new_oxygen, center)
    rel_b = minus(new_first, center)
    rel_c = minus(new_second, center)
    normal = cross_product(old_b, old_c)
    side = cross_product(rel_a, normal)
    upward = cross_product(normal, side)

    def normed(vector):
        size = jnp.sqrt(inner(vector, vector))
        return [a / size for a in vector]

    axis_z = normed(normal)
    axis_x = normed(side)
    axis_y = normed(upward)
    oldb_x = inner(axis_x, old_b)
    oldb_y = inner(axis_y, old_b)
    oldc_x = inner(axis_x, old_c)
    oldc_y = inner(axis_y, old_c)
    newa_z = inner(axis_z, rel_a)
    newb_x = inner(axis_x, rel_b)
    newb_y = inner(axis_y, rel_b)
    newb_z = inner(axis_z, rel_b)
    newc_x = inner(axis_x, rel_c)
    newc_y = inner(axis_y, rel_c)
    newc_z = inner(axis_z, rel_c)
    sin_phi = newa_z / oxygen_reach
    cos_phi = jnp.sqrt(1.0 - sin_phi * sin_phi)
    sin_psi = (newb_z - newc_z) / (2.0 * half_pair * cos_phi)
    cos_psi = jnp.sqrt(1.0 - sin_psi * sin_psi)
    rest_ay = oxygen_reach * cos_phi
    rest_bx = -half_pair * cos_psi
    lowered = -hydrogen_reach * cos_phi
    tilted = half_pair * sin_psi * sin_phi
    rest_by = lowered - tilted
    rest_cy = lowered + tilted
    alpha = rest_bx * (oldb_x - oldc_x) + oldb_y * rest_by + oldc_y * rest_cy
    beta = rest_bx * (oldc_y - oldb_y) + oldb_x * rest_by + oldc_x * rest_cy
    gamma = oldb_x * newb_y - newb_x * oldb_y + oldc_x * newc_y - newc_x * oldc_y
    summed = alpha * alpha + beta * beta
    sin_theta = (alpha * gamma - beta * jnp.sqrt(summed - gamma * gamma)) / summed
    cos_theta = jnp.sqrt(1.0 - sin_theta * sin_theta)
    final_ax = -rest_ay * sin_theta
    final_ay = rest_ay * cos_theta
    final_bx = rest_bx * cos_theta - rest_by * sin_theta
    final_by = rest_bx * sin_theta + rest_by * cos_theta
    final_cx = -rest_bx * cos_theta - rest_cy * sin_theta
    final_cy = -rest_bx * sin_theta + rest_cy * cos_theta

    def placed(x, y, z):
        return [
            center[c] + axis_x[c] * x + axis_y[c] * y + axis_z[c] * z for c in range(3)
        ]

    return (
        placed(final_ax, final_ay, newa_z)
        + placed(final_bx, final_by, newb_z)
        + placed(final_cx, final_cy, newc_z)
    )


def rounded(x):
    return x.astype(jnp.bfloat16).astype(jnp.float32)


def limbs(x, count):
    parts = []
    for _ in range(count - 1):
        part = rounded(x)
        parts.append(part)
        x = x - part
    return parts + [x]


def dot(a, b):
    return lax.dot_general(
        a, b, (((1,), (0,)), ((), ())), preferred_element_type=jnp.float32
    )


def row_sum(x):
    return jnp.sum(x, axis=0, keepdims=True)


def kernel(
    n, axis, pos, vel, mass, bonds, left, right, wpos, wvel, out_p, out_w,
    pos_x, vel_x, mass_x, bonds_x, left_x, right_x,
    index_s, table_s, scatter_s, gather_s, weight_s, hot_s,
    size_s, scale_s, gap_s, rhs_s, total_s, water_s,
    send_sem, recv_sem,
):
    atoms = pos.shape[1]
    lanes = atoms // SUB
    shift = lanes.bit_length() - 1
    bond_rows = bonds.shape[1] // LANES
    halo_rows = left.shape[0]
    rows = bond_rows + halo_rows
    water_rows = wpos.shape[1] // LANES

    own = (pos, vel, mass, bonds, left, right)
    others = (pos_x, vel_x, mass_x, bonds_x, left_x, right_x)
    me = lax.axis_index(axis)
    copies = []
    if n > 1:
        barrier = pltpu.get_barrier_semaphore()
        for k in range(1, n):
            peer = lax.rem(me + k, n)
            pl.semaphore_signal(
                barrier, inc=1, device_id={axis: peer},
                device_id_type=pl.DeviceIdType.MESH,
            )
        pl.semaphore_wait(barrier, n - 1)
        for k in range(1, n):
            peer = lax.rem(me + n - k, n)
            for t in range(len(own)):
                copy = pltpu.make_async_remote_copy(
                    src_ref=own[t],
                    dst_ref=others[t].at[k - 1],
                    send_sem=send_sem.at[k - 1, t],
                    recv_sem=recv_sem.at[k - 1, t],
                    device_id={axis: peer},
                    device_id_type=pl.DeviceIdType.MESH,
                )
                copy.start()
                copies.append(copy)

    components = wpos.shape[0]
    for source, base in ((wpos, 0), (wvel, components)):
        for c in range(components):
            for r in range(water_rows):
                water_s[base + c, pl.ds(r, 1), :] = source[
                    pl.ds(c, 1), pl.ds(r * LANES, LANES)
                ]
    before = [water_s[c] for c in range(components)]
    speed = [water_s[components + c] for c in range(components)]
    after = [b + time_step * v for b, v in zip(before, speed)]
    settled = settle(before, after)
    for c in range(components):
        water_s[c] = speed[c] + (settled[c] - after[c]) / time_step
    for c in range(components):
        for r in range(water_rows):
            out_w[pl.ds(c, 1), pl.ds(r * LANES, LANES)] = water_s[c, pl.ds(r, 1), :]

    def data(k):
        return own if k == 0 else tuple(ref.at[k - 1] for ref in others)

    def masses(k):
        ref = data(k)[2]
        step = lanes // LANES
        return jnp.concatenate(
            [ref[pl.ds(h, SUB, stride=step), :] for h in range(step)], axis=1
        )

    def index_bonds(k):
        ref = data(k)[3]
        for r in range(bond_rows):
            for e in range(2):
                index_s[k, pl.ds(2 * r + e, 1), :] = ref[
                    pl.ds(e, 1), pl.ds(r * LANES, LANES)
                ]

    def index_cross(k):
        for r in range(halo_rows):
            for e, ref in ((0, data(k)[5]), (1, data(k)[4])):
                index_s[k, pl.ds(2 * (bond_rows + r) + e, 1), :] = ref[pl.ds(r, 1), :]

    def one_hots(k):
        lane = (index_s[k] & (lanes - 1)).astype(jnp.float32)
        turned = lane.T.astype(jnp.bfloat16)
        along = lax.broadcasted_iota(jnp.int32, (LANES, LANES), 1).astype(jnp.float32)
        along = along.astype(jnp.bfloat16)
        down = lax.broadcasted_iota(jnp.int32, (lanes, LANES), 0).astype(jnp.float32)
        down = down.astype(jnp.bfloat16)
        one, zero = jnp.bfloat16(1.0), jnp.bfloat16(0.0)
        for h in range(2 * rows):
            flat = jnp.broadcast_to(lane[h:h + 1], (lanes, LANES)).astype(jnp.bfloat16)
            gather_s[k, :, pl.ds(h * LANES, LANES)] = jnp.where(
                down == flat, one, zero
            ).astype(F8)
            tall = jnp.broadcast_to(turned[:, h:h + 1], (LANES, LANES))
            for q in range(lanes // LANES):
                scatter_s[k, pl.ds(h * LANES, LANES), pl.ds(q * LANES, LANES)] = (
                    jnp.where(along + jnp.bfloat16(q * LANES) == tall, one, zero).astype(F8)
                )

    sub_iota = lax.broadcasted_iota(jnp.int32, (SUB, LANES), 0)

    def hot(k, r, e):
        index = index_s[k, pl.ds(2 * r + e, 1), :]
        return sub_iota == (index >> shift)

    def tables(k):
        position, velocity = data(k)[0], data(k)[1]
        for t, ref in ((0, position), (3, velocity)):
            for c in range(3):
                for r in range(SUB):
                    for q in range(lanes // LANES):
                        table_s[k, pl.ds((t + c) * SUB + r, 1), pl.ds(q * LANES, LANES)] = ref[
                            pl.ds(c, 1), pl.ds(r * lanes + q * LANES, LANES)
                        ]
        place = limbs(table_s[k, pl.ds(0, 3 * SUB), :], 3)
        speed = limbs(table_s[k, pl.ds(3 * SUB, 3 * SUB), :], 2)
        inverse = limbs(masses(k), 2)
        return jnp.concatenate(place + speed + inverse, axis=0)

    def ends(k, stacked, r):
        out = dot(stacked, gather_s[k, :, pl.ds(r * WIDE, WIDE)])

        def take(first, count):
            step = 3 * SUB if first < 15 * SUB else SUB
            total = out[first:first + step]
            for t in range(1, count):
                total = total + out[first + t * step:first + (t + 1) * step]
            return total

        place, speed, inverse = take(0, 3), take(9 * SUB, 2), take(15 * SUB, 2)
        pieces = [place[c * SUB:(c + 1) * SUB] for c in range(3)]
        pieces += [speed[c * SUB:(c + 1) * SUB] for c in range(3)] + [inverse]
        found = []
        for e in range(2):
            mask = hot(k, r, e)
            found.append(
                [jnp.where(mask, p[:, e * LANES:(e + 1) * LANES], 0.0) for p in pieces]
            )
        return found

    def start(k, r, at_i, at_j):
        diff = [row_sum(a - b) for a, b in zip(at_i[0:3], at_j[0:3])]
        rate = [row_sum(a - b) for a, b in zip(at_i[3:6], at_j[3:6])]
        size = jnp.sqrt(inner(diff, diff))
        unit = [d / size for d in diff]
        scale = 1.0 / jnp.sqrt(row_sum(at_i[6] + at_j[6]))
        gap = [d + time_step * v for d, v in zip(diff, rate)]
        size_s[k, pl.ds(r, 1), :] = size
        scale_s[k, pl.ds(r, 1), :] = scale
        for c in range(3):
            gap_s[k, c, pl.ds(r, 1), :] = gap[c]
        rhs_s[k, pl.ds(r, 1), :] = scale * (inner(unit, gap) - size)
        where = (k, k if r < bond_rows else (k + 1) % n)
        for e, sign in ((0, 1.0), (1, -1.0)):
            signed = jnp.where(hot(where[e], r, e), sign, 0.0)
            hot_s[where[e], r, e] = signed
            for c in range(3):
                weight_s[where[e], r, e, c] = signed * (scale * unit[c])

    for copy in copies:
        copy.wait()
    for k in range(n):
        index_bonds(k)
        index_cross(k)
        one_hots(k)
    cross = {}
    for k in range(n):
        stacked = tables(k)
        for r in range(rows):
            at_i, at_j = ends(k, stacked, r)
            if r < bond_rows:
                start(k, r, at_i, at_j)
            else:
                cross[k, r, 0] = at_i
                cross[(k + n - 1) % n, r, 1] = at_j
    for k in range(n):
        for r in range(bond_rows, rows):
            start(k, r, cross[k, r, 0], cross[k, r, 1])

    every = [(k, r) for k in range(n) for r in range(rows)]

    def constraint(k, r, e):
        return (k, r) if e == 0 or r < bond_rows else ((k + n - 1) % n, r)

    def scatter(k, x):
        chains = [None, None]
        for r in range(rows):
            columns = []
            for e in range(2):
                value = x[constraint(k, r, e)]
                high = [value * weight_s[k, r, e, c] for c in range(3)]
                low = [h - rounded(h) for h in high]
                columns.append(jnp.concatenate(high + low, axis=0))
            part = dot(
                jnp.concatenate(columns, axis=1), scatter_s[k, pl.ds(r * WIDE, WIDE), :]
            )
            chains[r % 2] = part if chains[r % 2] is None else chains[r % 2] + part
        summed = chains[0] + chains[1]
        weight = masses(k)
        return [
            weight * (summed[c * SUB:(c + 1) * SUB] + summed[(3 + c) * SUB:(4 + c) * SUB])
            for c in range(3)
        ]

    def gather(k, field):
        stacked = jnp.concatenate(field + [f - rounded(f) for f in field], axis=0)
        found = []
        for r in range(rows):
            out = dot(stacked, gather_s[k, :, pl.ds(r * WIDE, WIDE)])
            both = out[:3 * SUB] + out[3 * SUB:]
            found.append([
                [both[c * SUB:(c + 1) * SUB, e * LANES:(e + 1) * LANES] for c in range(3)]
                for e in range(2)
            ])
        return found

    def at_constraints(found, function):
        partial = {}
        for k in range(n):
            for r in range(rows):
                for e in range(2):
                    partial[constraint(k, r, e) + (e,)] = function(k, r, e, found[k][r][e])
        return partial

    def apply(rhs, x):
        fields = [scatter(k, x) for k in range(n)]
        found = [gather(k, fields[k]) for k in range(n)]
        parts = at_constraints(
            found,
            lambda k, r, e, f: inner([weight_s[k, r, e, c] for c in range(3)], f),
        )
        return {
            (k, r): rhs[k, r] + x[k, r] - row_sum(parts[k, r, 0] + parts[k, r, 1])
            for k, r in every
        }

    def expand(rhs):
        if n > 2:
            return lax.fori_loop(0, ORDER, lambda _, x: apply(rhs, x), rhs)
        x = rhs
        for _ in range(ORDER):
            x = apply(rhs, x)
        return x

    def load_rhs():
        return {(k, r): rhs_s[k, pl.ds(r, 1), :] for k, r in every}

    for c in range(3):
        total_s[c] = jnp.zeros((SUB, lanes), jnp.float32)

    def one_round(_, carry):
        x = expand(load_rhs())
        fields = [scatter(k, x) for k in range(n)]
        for c in range(3):
            total_s[c] = total_s[c] + fields[0][c]
        found = [gather(k, fields[k]) for k in range(n)]
        parts = at_constraints(
            found, lambda k, r, e, f: [hot_s[k, r, e] * f[c] for c in range(3)]
        )
        for k, r in every:
            gap = []
            for c in range(3):
                moved = row_sum(parts[k, r, 0][c] + parts[k, r, 1][c])
                gap.append(gap_s[k, c, pl.ds(r, 1), :] - moved)
                gap_s[k, c, pl.ds(r, 1), :] = gap[c]
            size = size_s[k, pl.ds(r, 1), :]
            scale = scale_s[k, pl.ds(r, 1), :]
            rhs_s[k, pl.ds(r, 1), :] = scale * (
                size - jnp.sqrt(2.0 * size * size - inner(gap, gap))
            )
        return carry

    lax.fori_loop(0, ITER, one_round, 0)
    last = scatter(0, expand(load_rhs()))
    for c in range(3):
        total_s[c] = (total_s[c] + last[c]) / time_step
    for c in range(3):
        for r in range(SUB):
            for q in range(lanes // LANES):
                cols = pl.ds(r * lanes + q * LANES, LANES)
                out_p[pl.ds(c, 1), cols] = (
                    vel[pl.ds(c, 1), cols]
                    - total_s[c, pl.ds(r, 1), pl.ds(q * LANES, LANES)]
                )


def on_device(
    n, protein_pos, protein_vel, inv_mass, bond_atoms, left_atoms, right_atoms, water_pos, water_vel
):
    atoms = protein_pos.shape[1]
    lanes = atoms // SUB
    halo_rows = left_atoms.shape[0] // LANES
    rows = bond_atoms.shape[1] // LANES + halo_rows
    packed = -(-rows // SUB) * SUB
    ends = -(-2 * rows // SUB) * SUB
    others = max(n - 1, 1)
    mass = inv_mass.reshape(atoms // LANES, LANES)
    left = left_atoms.reshape(halo_rows, LANES)
    right = right_atoms.reshape(halo_rows, LANES)
    operands = (protein_pos, protein_vel, mass, bond_atoms, left, right, water_pos, water_vel)
    vmem = pl.BlockSpec(memory_space=pltpu.VMEM)
    return pl.pallas_call(
        functools.partial(kernel, n, "dom"),
        out_shape=(
            jax.ShapeDtypeStruct(protein_vel.shape, jnp.float32),
            jax.ShapeDtypeStruct(water_vel.shape, jnp.float32),
        ),
        in_specs=[vmem] * len(operands),
        out_specs=(vmem, vmem),
        scratch_shapes=[
            pltpu.VMEM((others,) + x.shape, x.dtype) for x in operands[:6]
        ] + [
            pltpu.VMEM((n, ends, LANES), jnp.int32),
            pltpu.VMEM((n, 6 * SUB, lanes), jnp.float32),
            pltpu.VMEM((n, rows * WIDE, lanes), F8),
            pltpu.VMEM((n, lanes, rows * WIDE), F8),
            pltpu.VMEM((n, rows, 2, 3, SUB, LANES), jnp.float32),
            pltpu.VMEM((n, rows, 2, SUB, LANES), jnp.float32),
            pltpu.VMEM((n, packed, LANES), jnp.float32),
            pltpu.VMEM((n, packed, LANES), jnp.float32),
            pltpu.VMEM((n, 3, packed, LANES), jnp.float32),
            pltpu.VMEM((n, packed, LANES), jnp.float32),
            pltpu.VMEM((3, SUB, lanes), jnp.float32),
            pltpu.VMEM((2 * water_pos.shape[0], water_pos.shape[1] // LANES, LANES), jnp.float32),
            pltpu.SemaphoreType.DMA((others, 6)),
            pltpu.SemaphoreType.DMA((others, 6)),
        ],
        compiler_params=pltpu.CompilerParams(
            collective_id=0, has_side_effects=True, vmem_limit_bytes=60 * 1024 * 1024
        ),
    )(*operands)


def solution(mesh):
    in_specs = (
        P(None, ("rep", "dom")),
        P(None, ("rep", "dom")),
        P(("rep", "dom")),
        P(None, ("rep", "dom")),
        P(("rep", "dom")),
        P(("rep", "dom")),
        P(None, ("rep", "dom")),
        P(None, ("rep", "dom")),
    )
    out_specs = (P(None, ("rep", "dom")), P(None, ("rep", "dom")))
    return jax.shard_map(
        functools.partial(on_device, mesh.shape["dom"]),
        mesh=mesh, in_specs=in_specs, out_specs=out_specs, check_vma=False,
    )
```

```python
import functools
import math

import jax
import jax.numpy as jnp
from jax import lax
from jax.experimental import pallas as pl
from jax.experimental.pallas import tpu as pltpu
from jax.sharding import PartitionSpec as P

ORDER = 4
ITER = 2
LANES = 128
SUB = 8
WIDE = 2 * LANES
F8 = jnp.float8_e4m3fn


time_step = 0.002
mass_oxygen = 15.9994
mass_hydrogen = 1.008
oxygen_hydrogen = 0.09572
hydrogen_pair = 0.15139
total_mass = mass_oxygen + 2.0 * mass_hydrogen
half_pair = 0.5 * hydrogen_pair
water_height = math.sqrt(oxygen_hydrogen * oxygen_hydrogen - half_pair * half_pair)
oxygen_reach = 2.0 * mass_hydrogen * water_height / total_mass
hydrogen_reach = water_height - oxygen_reach


def cross_product(left, right):
    return [
        left[1] * right[2] - left[2] * right[1],
        left[2] * right[0] - left[0] * right[2],
        left[0] * right[1] - left[1] * right[0],
    ]


def inner(left, right):
    return left[0] * right[0] + left[1] * right[1] + left[2] * right[2]


def minus(left, right):
    return [a - b for a, b in zip(left, right)]


def settle(before, after):
    old_oxygen, old_first, old_second = (before[0:3], before[3:6], before[6:9])
    new_oxygen, new_first, new_second = (after[0:3], after[3:6], after[6:9])
    center = [
        (mass_oxygen * o + mass_hydrogen * (f + s)) / total_mass
        for o, f, s in zip(new_oxygen, new_first, new_second)
    ]
    old_b = minus(old_first, old_oxygen)
    old_c = minus(old_second, old_oxygen)
    rel_a = minus(new_oxygen, center)
    rel_b = minus(new_first, center)
    rel_c = minus(new_second, center)
    normal = cross_product(old_b, old_c)
    side = cross_product(rel_a, normal)
    upward = cross_product(normal, side)

    def normed(vector):
        size = jnp.sqrt(inner(vector, vector))
        return [a / size for a in vector]

    axis_z = normed(normal)
    axis_x = normed(side)
    axis_y = normed(upward)
    oldb_x = inner(axis_x, old_b)
    oldb_y = inner(axis_y, old_b)
    oldc_x = inner(axis_x, old_c)
    oldc_y = inner(axis_y, old_c)
    newa_z = inner(axis_z, rel_a)
    newb_x = inner(axis_x, rel_b)
    newb_y = inner(axis_y, rel_b)
    newb_z = inner(axis_z, rel_b)
    newc_x = inner(axis_x, rel_c)
    newc_y = inner(axis_y, rel_c)
    newc_z = inner(axis_z, rel_c)
    sin_phi = newa_z / oxygen_reach
    cos_phi = jnp.sqrt(1.0 - sin_phi * sin_phi)
    sin_psi = (newb_z - newc_z) / (2.0 * half_pair * cos_phi)
    cos_psi = jnp.sqrt(1.0 - sin_psi * sin_psi)
    rest_ay = oxygen_reach * cos_phi
    rest_bx = -half_pair * cos_psi
    lowered = -hydrogen_reach * cos_phi
    tilted = half_pair * sin_psi * sin_phi
    rest_by = lowered - tilted
    rest_cy = lowered + tilted
    alpha = rest_bx * (oldb_x - oldc_x) + oldb_y * rest_by + oldc_y * rest_cy
    beta = rest_bx * (oldc_y - oldb_y) + oldb_x * rest_by + oldc_x * rest_cy
    gamma = oldb_x * newb_y - newb_x * oldb_y + oldc_x * newc_y - newc_x * oldc_y
    summed = alpha * alpha + beta * beta
    sin_theta = (alpha * gamma - beta * jnp.sqrt(summed - gamma * gamma)) / summed
    cos_theta = jnp.sqrt(1.0 - sin_theta * sin_theta)
    final_ax = -rest_ay * sin_theta
    final_ay = rest_ay * cos_theta
    final_bx = rest_bx * cos_theta - rest_by * sin_theta
    final_by = rest_bx * sin_theta + rest_by * cos_theta
    final_cx = -rest_bx * cos_theta - rest_cy * sin_theta
    final_cy = -rest_bx * sin_theta + rest_cy * cos_theta

    def placed(x, y, z):
        return [
            center[c] + axis_x[c] * x + axis_y[c] * y + axis_z[c] * z for c in range(3)
        ]

    return (
        placed(final_ax, final_ay, newa_z)
        + placed(final_bx, final_by, newb_z)
        + placed(final_cx, final_cy, newc_z)
    )


def rounded(x):
    return x.astype(jnp.bfloat16).astype(jnp.float32)


def limbs(x, count):
    parts = []
    for _ in range(count - 1):
        part = rounded(x)
        parts.append(part)
        x = x - part
    return parts + [x]


def dot(a, b):
    return lax.dot_general(
        a, b, (((1,), (0,)), ((), ())), preferred_element_type=jnp.float32
    )


def row_sum(x):
    return jnp.sum(x, axis=0, keepdims=True)


def kernel(
    n, axis, *refs
):
    given, refs = refs[:8], refs[8:]
    out_p, out_w = refs[:2]
    pos, vel, mass, bonds, left, right, wpos, wvel = refs[2:10]
    pos_x, vel_x, mass_x, bonds_x, left_x, right_x = refs[10:16]
    (
    index_s, table_s, scatter_s, gather_s, weight_s, hot_s,
    size_s, scale_s, gap_s, rhs_s, total_s, water_s,
    load_sem, send_sem, recv_sem,
    ) = refs[16:]
    atoms = pos.shape[1]
    lanes = atoms // SUB
    shift = lanes.bit_length() - 1
    bond_rows = bonds.shape[1] // LANES
    halo_rows = left.shape[0]
    rows = bond_rows + halo_rows
    water_rows = wpos.shape[1] // LANES

    own = (pos, vel, mass, bonds, left, right)
    others = (pos_x, vel_x, mass_x, bonds_x, left_x, right_x)
    me = lax.axis_index(axis)
    loads = [
        pltpu.make_async_copy(source, to, load_sem.at[t])
        for t, (source, to) in enumerate(zip(given, own + (wpos, wvel)))
    ]
    for load in loads:
        load.start()
    copies = []
    if n > 1:
        barrier = pltpu.get_barrier_semaphore()
        for k in range(1, n):
            peer = lax.rem(me + k, n)
            pl.semaphore_signal(
                barrier, inc=1, device_id={axis: peer},
                device_id_type=pl.DeviceIdType.MESH,
            )
    for load in loads[:len(own)]:
        load.wait()
    if n > 1:
        pl.semaphore_wait(barrier, n - 1)
        for k in range(1, n):
            peer = lax.rem(me + n - k, n)
            for t in range(len(own)):
                copy = pltpu.make_async_remote_copy(
                    src_ref=own[t],
                    dst_ref=others[t].at[k - 1],
                    send_sem=send_sem.at[k - 1, t],
                    recv_sem=recv_sem.at[k - 1, t],
                    device_id={axis: peer},
                    device_id_type=pl.DeviceIdType.MESH,
                )
                copy.start()
                copies.append(copy)

    for load in loads[len(own):]:
        load.wait()
    components = wpos.shape[0]
    for source, base in ((wpos, 0), (wvel, components)):
        for c in range(components):
            for r in range(water_rows):
                water_s[base + c, pl.ds(r, 1), :] = source[
                    pl.ds(c, 1), pl.ds(r * LANES, LANES)
                ]
    before = [water_s[c] for c in range(components)]
    speed = [water_s[components + c] for c in range(components)]
    after = [b + time_step * v for b, v in zip(before, speed)]
    settled = settle(before, after)
    for c in range(components):
        water_s[c] = speed[c] + (settled[c] - after[c]) / time_step
    for c in range(components):
        for r in range(water_rows):
            out_w[pl.ds(c, 1), pl.ds(r * LANES, LANES)] = water_s[c, pl.ds(r, 1), :]

    def data(k):
        return own if k == 0 else tuple(ref.at[k - 1] for ref in others)

    def masses(k):
        ref = data(k)[2]
        step = lanes // LANES
        return jnp.concatenate(
            [ref[pl.ds(h, SUB, stride=step), :] for h in range(step)], axis=1
        )

    def index_bonds(k):
        ref = data(k)[3]
        for r in range(bond_rows):
            for e in range(2):
                index_s[k, pl.ds(2 * r + e, 1), :] = ref[
                    pl.ds(e, 1), pl.ds(r * LANES, LANES)
                ]

    def index_cross(k):
        for r in range(halo_rows):
            for e, ref in ((0, data(k)[5]), (1, data(k)[4])):
                index_s[k, pl.ds(2 * (bond_rows + r) + e, 1), :] = ref[pl.ds(r, 1), :]

    def one_hots(k):
        lane = (index_s[k] & (lanes - 1)).astype(jnp.float32)
        turned = lane.T.astype(jnp.bfloat16)
        along = lax.broadcasted_iota(jnp.int32, (LANES, LANES), 1).astype(jnp.float32)
        along = along.astype(jnp.bfloat16)
        down = lax.broadcasted_iota(jnp.int32, (lanes, LANES), 0).astype(jnp.float32)
        down = down.astype(jnp.bfloat16)
        one, zero = jnp.bfloat16(1.0), jnp.bfloat16(0.0)
        for h in range(2 * rows):
            flat = jnp.broadcast_to(lane[h:h + 1], (lanes, LANES)).astype(jnp.bfloat16)
            gather_s[k, :, pl.ds(h * LANES, LANES)] = jnp.where(
                down == flat, one, zero
            ).astype(F8)
            tall = jnp.broadcast_to(turned[:, h:h + 1], (LANES, LANES))
            for q in range(lanes // LANES):
                scatter_s[k, pl.ds(h * LANES, LANES), pl.ds(q * LANES, LANES)] = (
                    jnp.where(along + jnp.bfloat16(q * LANES) == tall, one, zero).astype(F8)
                )

    sub_iota = lax.broadcasted_iota(jnp.int32, (SUB, LANES), 0)

    def hot(k, r, e):
        index = index_s[k, pl.ds(2 * r + e, 1), :]
        return sub_iota == (index >> shift)

    def tables(k):
        position, velocity = data(k)[0], data(k)[1]
        for t, ref in ((0, position), (3, velocity)):
            for c in range(3):
                for r in range(SUB):
                    for q in range(lanes // LANES):
                        table_s[k, pl.ds((t + c) * SUB + r, 1), pl.ds(q * LANES, LANES)] = ref[
                            pl.ds(c, 1), pl.ds(r * lanes + q * LANES, LANES)
                        ]
        place = limbs(table_s[k, pl.ds(0, 3 * SUB), :], 3)
        speed = limbs(table_s[k, pl.ds(3 * SUB, 3 * SUB), :], 2)
        inverse = limbs(masses(k), 2)
        return jnp.concatenate(place + speed + inverse, axis=0)

    def ends(k, stacked, r):
        out = dot(stacked, gather_s[k, :, pl.ds(r * WIDE, WIDE)])

        def take(first, count):
            step = 3 * SUB if first < 15 * SUB else SUB
            total = out[first:first + step]
            for t in range(1, count):
                total = total + out[first + t * step:first + (t + 1) * step]
            return total

        place, speed, inverse = take(0, 3), take(9 * SUB, 2), take(15 * SUB, 2)
        pieces = [place[c * SUB:(c + 1) * SUB] for c in range(3)]
        pieces += [speed[c * SUB:(c + 1) * SUB] for c in range(3)] + [inverse]
        found = []
        for e in range(2):
            mask = hot(k, r, e)
            found.append(
                [jnp.where(mask, p[:, e * LANES:(e + 1) * LANES], 0.0) for p in pieces]
            )
        return found

    def start(k, r, at_i, at_j):
        diff = [row_sum(a - b) for a, b in zip(at_i[0:3], at_j[0:3])]
        rate = [row_sum(a - b) for a, b in zip(at_i[3:6], at_j[3:6])]
        size = jnp.sqrt(inner(diff, diff))
        unit = [d / size for d in diff]
        scale = 1.0 / jnp.sqrt(row_sum(at_i[6] + at_j[6]))
        gap = [d + time_step * v for d, v in zip(diff, rate)]
        size_s[k, pl.ds(r, 1), :] = size
        scale_s[k, pl.ds(r, 1), :] = scale
        for c in range(3):
            gap_s[k, c, pl.ds(r, 1), :] = gap[c]
        rhs_s[k, pl.ds(r, 1), :] = scale * (inner(unit, gap) - size)
        where = (k, k if r < bond_rows else (k + 1) % n)
        for e, sign in ((0, 1.0), (1, -1.0)):
            signed = jnp.where(hot(where[e], r, e), sign, 0.0)
            hot_s[where[e], r, e] = signed
            for c in range(3):
                weight_s[where[e], r, e, c] = signed * (scale * unit[c])

    cross = {}

    def prepare(k):
        index_bonds(k)
        index_cross(k)
        one_hots(k)
        stacked = tables(k)
        for r in range(rows):
            at_i, at_j = ends(k, stacked, r)
            if r < bond_rows:
                start(k, r, at_i, at_j)
            else:
                cross[k, r, 0] = at_i
                cross[(k + n - 1) % n, r, 1] = at_j

    prepare(0)
    for copy in copies:
        copy.wait()
    for k in range(1, n):
        prepare(k)
    for k in range(n):
        for r in range(bond_rows, rows):
            start(k, r, cross[k, r, 0], cross[k, r, 1])

    every = [(k, r) for k in range(n) for r in range(rows)]

    def constraint(k, r, e):
        return (k, r) if e == 0 or r < bond_rows else ((k + n - 1) % n, r)

    def scatter(k, x):
        chains = [None, None]
        for r in range(rows):
            columns = []
            for e in range(2):
                value = x[constraint(k, r, e)]
                high = [value * weight_s[k, r, e, c] for c in range(3)]
                low = [h - rounded(h) for h in high]
                columns.append(jnp.concatenate(high + low, axis=0))
            part = dot(
                jnp.concatenate(columns, axis=1), scatter_s[k, pl.ds(r * WIDE, WIDE), :]
            )
            chains[r % 2] = part if chains[r % 2] is None else chains[r % 2] + part
        weight = masses(k)
        pieces = [
            [
                weight * (p[c * SUB:(c + 1) * SUB] + p[(3 + c) * SUB:(4 + c) * SUB])
                for c in range(3)
            ]
            for p in chains
        ]
        return [a + b for a, b in zip(*pieces)]

    def gather(k, field):
        stacked = jnp.concatenate(field + [f - rounded(f) for f in field], axis=0)
        found = []
        for r in range(rows):
            out = dot(stacked, gather_s[k, :, pl.ds(r * WIDE, WIDE)])
            both = out[:3 * SUB] + out[3 * SUB:]
            found.append([
                [both[c * SUB:(c + 1) * SUB, e * LANES:(e + 1) * LANES] for c in range(3)]
                for e in range(2)
            ])
        return found

    def at_constraints(found, function):
        partial = {}
        for k in range(n):
            for r in range(rows):
                for e in range(2):
                    partial[constraint(k, r, e) + (e,)] = function(k, r, e, found[k][r][e])
        return partial

    def apply(rhs, x):
        fields = [scatter(k, x) for k in range(n)]
        found = [gather(k, fields[k]) for k in range(n)]
        parts = at_constraints(
            found,
            lambda k, r, e, f: inner([weight_s[k, r, e, c] for c in range(3)], f),
        )
        return {
            (k, r): rhs[k, r] + x[k, r] - row_sum(parts[k, r, 0] + parts[k, r, 1])
            for k, r in every
        }

    def expand(rhs):
        if n > 2:
            return lax.fori_loop(0, ORDER, lambda _, x: apply(rhs, x), rhs)
        x = rhs
        for _ in range(ORDER):
            x = apply(rhs, x)
        return x

    def load_rhs():
        return {(k, r): rhs_s[k, pl.ds(r, 1), :] for k, r in every}

    for c in range(3):
        total_s[c] = jnp.zeros((SUB, lanes), jnp.float32)

    def one_round(_, carry):
        x = expand(load_rhs())
        fields = [scatter(k, x) for k in range(n)]
        for c in range(3):
            total_s[c] = total_s[c] + fields[0][c]
        found = [gather(k, fields[k]) for k in range(n)]
        parts = at_constraints(
            found, lambda k, r, e, f: [hot_s[k, r, e] * f[c] for c in range(3)]
        )
        for k, r in every:
            gap = []
            for c in range(3):
                moved = row_sum(parts[k, r, 0][c] + parts[k, r, 1][c])
                gap.append(gap_s[k, c, pl.ds(r, 1), :] - moved)
                gap_s[k, c, pl.ds(r, 1), :] = gap[c]
            size = size_s[k, pl.ds(r, 1), :]
            scale = scale_s[k, pl.ds(r, 1), :]
            rhs_s[k, pl.ds(r, 1), :] = scale * (
                size - jnp.sqrt(2.0 * size * size - inner(gap, gap))
            )
        return carry

    lax.fori_loop(0, ITER, one_round, 0)
    last = scatter(0, expand(load_rhs()))
    for c in range(3):
        total_s[c] = (total_s[c] + last[c]) / time_step
    for c in range(3):
        for r in range(SUB):
            for q in range(lanes // LANES):
                cols = pl.ds(r * lanes + q * LANES, LANES)
                out_p[pl.ds(c, 1), cols] = (
                    vel[pl.ds(c, 1), cols]
                    - total_s[c, pl.ds(r, 1), pl.ds(q * LANES, LANES)]
                )


def hand_over(p, w, out_p, out_w):
    out_p[...] = p[...]
    out_w[...] = w[...]


def on_device(
    n, protein_pos, protein_vel, inv_mass, bond_atoms, left_atoms, right_atoms, water_pos, water_vel
):
    atoms = protein_pos.shape[1]
    lanes = atoms // SUB
    halo_rows = left_atoms.shape[0] // LANES
    rows = bond_atoms.shape[1] // LANES + halo_rows
    packed = -(-rows // SUB) * SUB
    ends = -(-2 * rows // SUB) * SUB
    others = max(n - 1, 1)
    mass = inv_mass.reshape(atoms // LANES, LANES)
    left = left_atoms.reshape(halo_rows, LANES)
    right = right_atoms.reshape(halo_rows, LANES)
    operands = (protein_pos, protein_vel, mass, bond_atoms, left, right, water_pos, water_vel)
    vmem = pl.BlockSpec(memory_space=pltpu.VMEM)
    results = pl.pallas_call(
        functools.partial(kernel, n, "dom"),
        out_shape=(
            pltpu.VMEM(protein_vel.shape, jnp.float32),
            pltpu.VMEM(water_vel.shape, jnp.float32),
        ),
        in_specs=[pl.BlockSpec(memory_space=pltpu.HBM)] * len(operands),
        out_specs=(vmem, vmem),
        scratch_shapes=[pltpu.VMEM(x.shape, x.dtype) for x in operands] + [
            pltpu.VMEM((others,) + x.shape, x.dtype) for x in operands[:6]
        ] + [
            pltpu.VMEM((n, ends, LANES), jnp.int32),
            pltpu.VMEM((n, 6 * SUB, lanes), jnp.float32),
            pltpu.VMEM((n, rows * WIDE, lanes), F8),
            pltpu.VMEM((n, lanes, rows * WIDE), F8),
            pltpu.VMEM((n, rows, 2, 3, SUB, LANES), jnp.float32),
            pltpu.VMEM((n, rows, 2, SUB, LANES), jnp.float32),
            pltpu.VMEM((n, packed, LANES), jnp.float32),
            pltpu.VMEM((n, packed, LANES), jnp.float32),
            pltpu.VMEM((n, 3, packed, LANES), jnp.float32),
            pltpu.VMEM((n, packed, LANES), jnp.float32),
            pltpu.VMEM((3, SUB, lanes), jnp.float32),
            pltpu.VMEM((2 * water_pos.shape[0], water_pos.shape[1] // LANES, LANES), jnp.float32),
            pltpu.SemaphoreType.DMA((len(operands),)),
            pltpu.SemaphoreType.DMA((others, 6)),
            pltpu.SemaphoreType.DMA((others, 6)),
        ],
        compiler_params=pltpu.CompilerParams(
            collective_id=0, has_side_effects=True, vmem_limit_bytes=60 * 1024 * 1024
        ),
    )(*operands)
    return pl.pallas_call(
        hand_over,
        out_shape=[jax.ShapeDtypeStruct(x.shape, x.dtype) for x in results],
        in_specs=[vmem] * 2,
        out_specs=[vmem] * 2,
        compiler_params=pltpu.CompilerParams(vmem_limit_bytes=8 * 1024 * 1024),
    )(*results)


def solution(mesh):
    in_specs = (
        P(None, ("rep", "dom")),
        P(None, ("rep", "dom")),
        P(("rep", "dom")),
        P(None, ("rep", "dom")),
        P(("rep", "dom")),
        P(("rep", "dom")),
        P(None, ("rep", "dom")),
        P(None, ("rep", "dom")),
    )
    out_specs = (P(None, ("rep", "dom")), P(None, ("rep", "dom")))
    return jax.shard_map(
        functools.partial(on_device, mesh.shape["dom"]),
        mesh=mesh, in_specs=in_specs, out_specs=out_specs, check_vma=False,
    )
```

```python
import functools
import math

import jax
import jax.numpy as jnp
from jax import lax
from jax.experimental import pallas as pl
from jax.experimental.pallas import tpu as pltpu
from jax.sharding import PartitionSpec as P

ORDER = 4
ITER = 2
LANES = 128
SUB = 8
WIDE = 2 * LANES
F8 = jnp.float8_e4m3fn


time_step = 0.002
mass_oxygen = 15.9994
mass_hydrogen = 1.008
oxygen_hydrogen = 0.09572
hydrogen_pair = 0.15139
total_mass = mass_oxygen + 2.0 * mass_hydrogen
half_pair = 0.5 * hydrogen_pair
water_height = math.sqrt(oxygen_hydrogen * oxygen_hydrogen - half_pair * half_pair)
oxygen_reach = 2.0 * mass_hydrogen * water_height / total_mass
hydrogen_reach = water_height - oxygen_reach


def cross_product(left, right):
    return [
        left[1] * right[2] - left[2] * right[1],
        left[2] * right[0] - left[0] * right[2],
        left[0] * right[1] - left[1] * right[0],
    ]


def inner(left, right):
    return left[0] * right[0] + left[1] * right[1] + left[2] * right[2]


def minus(left, right):
    return [a - b for a, b in zip(left, right)]


def settle(before, after):
    old_oxygen, old_first, old_second = (before[0:3], before[3:6], before[6:9])
    new_oxygen, new_first, new_second = (after[0:3], after[3:6], after[6:9])
    center = [
        (mass_oxygen * o + mass_hydrogen * (f + s)) / total_mass
        for o, f, s in zip(new_oxygen, new_first, new_second)
    ]
    old_b = minus(old_first, old_oxygen)
    old_c = minus(old_second, old_oxygen)
    rel_a = minus(new_oxygen, center)
    rel_b = minus(new_first, center)
    rel_c = minus(new_second, center)
    normal = cross_product(old_b, old_c)
    side = cross_product(rel_a, normal)
    upward = cross_product(normal, side)

    def normed(vector):
        size = jnp.sqrt(inner(vector, vector))
        return [a / size for a in vector]

    axis_z = normed(normal)
    axis_x = normed(side)
    axis_y = normed(upward)
    oldb_x = inner(axis_x, old_b)
    oldb_y = inner(axis_y, old_b)
    oldc_x = inner(axis_x, old_c)
    oldc_y = inner(axis_y, old_c)
    newa_z = inner(axis_z, rel_a)
    newb_x = inner(axis_x, rel_b)
    newb_y = inner(axis_y, rel_b)
    newb_z = inner(axis_z, rel_b)
    newc_x = inner(axis_x, rel_c)
    newc_y = inner(axis_y, rel_c)
    newc_z = inner(axis_z, rel_c)
    sin_phi = newa_z / oxygen_reach
    cos_phi = jnp.sqrt(1.0 - sin_phi * sin_phi)
    sin_psi = (newb_z - newc_z) / (2.0 * half_pair * cos_phi)
    cos_psi = jnp.sqrt(1.0 - sin_psi * sin_psi)
    rest_ay = oxygen_reach * cos_phi
    rest_bx = -half_pair * cos_psi
    lowered = -hydrogen_reach * cos_phi
    tilted = half_pair * sin_psi * sin_phi
    rest_by = lowered - tilted
    rest_cy = lowered + tilted
    alpha = rest_bx * (oldb_x - oldc_x) + oldb_y * rest_by + oldc_y * rest_cy
    beta = rest_bx * (oldc_y - oldb_y) + oldb_x * rest_by + oldc_x * rest_cy
    gamma = oldb_x * newb_y - newb_x * oldb_y + oldc_x * newc_y - newc_x * oldc_y
    summed = alpha * alpha + beta * beta
    sin_theta = (alpha * gamma - beta * jnp.sqrt(summed - gamma * gamma)) / summed
    cos_theta = jnp.sqrt(1.0 - sin_theta * sin_theta)
    final_ax = -rest_ay * sin_theta
    final_ay = rest_ay * cos_theta
    final_bx = rest_bx * cos_theta - rest_by * sin_theta
    final_by = rest_bx * sin_theta + rest_by * cos_theta
    final_cx = -rest_bx * cos_theta - rest_cy * sin_theta
    final_cy = -rest_bx * sin_theta + rest_cy * cos_theta

    def placed(x, y, z):
        return [
            center[c] + axis_x[c] * x + axis_y[c] * y + axis_z[c] * z for c in range(3)
        ]

    return (
        placed(final_ax, final_ay, newa_z)
        + placed(final_bx, final_by, newb_z)
        + placed(final_cx, final_cy, newc_z)
    )


def rounded(x):
    return x.astype(jnp.bfloat16).astype(jnp.float32)


def limbs(x, count):
    parts = []
    for _ in range(count - 1):
        part = rounded(x)
        parts.append(part)
        x = x - part
    return parts + [x]


def dot(a, b):
    return lax.dot_general(
        a, b, (((1,), (0,)), ((), ())), preferred_element_type=jnp.float32
    )


def row_sum(x):
    return jnp.sum(x, axis=0, keepdims=True)


def kernel(
    n, axis, *refs
):
    given, refs = refs[:8], refs[8:]
    out_p, out_w = refs[:2]
    pos, vel, mass, bonds, left, right, wpos, wvel = refs[2:10]
    pos_x, vel_x, mass_x, bonds_x, left_x, right_x = refs[10:16]
    (
    index_s, table_s, scatter_s, gather_s, weight_s, hot_s,
    size_s, scale_s, gap_s, rhs_s, total_s, water_s,
    load_sem, send_sem, recv_sem,
    ) = refs[16:]
    atoms = pos.shape[1]
    lanes = atoms // SUB
    shift = lanes.bit_length() - 1
    bond_rows = bonds.shape[1] // LANES
    halo_rows = left.shape[0]
    rows = bond_rows + halo_rows
    water_rows = wpos.shape[1] // LANES

    own = (pos, vel, mass, bonds, left, right)
    others = (pos_x, vel_x, mass_x, bonds_x, left_x, right_x)
    me = lax.axis_index(axis)
    loads = [
        pltpu.make_async_copy(source, to, load_sem.at[t])
        for t, (source, to) in enumerate(zip(given, own + (wpos, wvel)))
    ]
    for load in loads:
        load.start()
    copies = []
    if n > 1:
        barrier = pltpu.get_barrier_semaphore()
        for k in range(1, n):
            peer = lax.rem(me + k, n)
            pl.semaphore_signal(
                barrier, inc=1, device_id={axis: peer},
                device_id_type=pl.DeviceIdType.MESH,
            )
    for load in loads[:len(own)]:
        load.wait()
    if n > 1:
        pl.semaphore_wait(barrier, n - 1)
        for k in range(1, n):
            peer = lax.rem(me + n - k, n)
            for t in range(len(own)):
                copy = pltpu.make_async_remote_copy(
                    src_ref=own[t],
                    dst_ref=others[t].at[k - 1],
                    send_sem=send_sem.at[k - 1, t],
                    recv_sem=recv_sem.at[k - 1, t],
                    device_id={axis: peer},
                    device_id_type=pl.DeviceIdType.MESH,
                )
                copy.start()
                copies.append(copy)

    for load in loads[len(own):]:
        load.wait()
    components = wpos.shape[0]
    for source, base in ((wpos, 0), (wvel, components)):
        for c in range(components):
            for r in range(water_rows):
                water_s[base + c, pl.ds(r, 1), :] = source[
                    pl.ds(c, 1), pl.ds(r * LANES, LANES)
                ]
    before = [water_s[c] for c in range(components)]
    speed = [water_s[components + c] for c in range(components)]
    after = [b + time_step * v for b, v in zip(before, speed)]
    settled = settle(before, after)
    for c in range(components):
        water_s[c] = speed[c] + (settled[c] - after[c]) / time_step
    for c in range(components):
        for r in range(water_rows):
            out_w[pl.ds(c, 1), pl.ds(r * LANES, LANES)] = water_s[c, pl.ds(r, 1), :]

    def data(k):
        return own if k == 0 else tuple(ref.at[k - 1] for ref in others)

    def masses(k):
        ref = data(k)[2]
        step = lanes // LANES
        return jnp.concatenate(
            [ref[pl.ds(h, SUB, stride=step), :] for h in range(step)], axis=1
        )

    def index_bonds(k):
        ref = data(k)[3]
        for r in range(bond_rows):
            for e in range(2):
                index_s[k, pl.ds(2 * r + e, 1), :] = ref[
                    pl.ds(e, 1), pl.ds(r * LANES, LANES)
                ]

    def index_cross(k):
        for r in range(halo_rows):
            for e, ref in ((0, data(k)[5]), (1, data(k)[4])):
                index_s[k, pl.ds(2 * (bond_rows + r) + e, 1), :] = ref[pl.ds(r, 1), :]

    def one_hots(k):
        lane = (index_s[k] & (lanes - 1)).astype(jnp.float32)
        turned = lane.T.astype(jnp.bfloat16)
        along = lax.broadcasted_iota(jnp.int32, (LANES, LANES), 1).astype(jnp.float32)
        along = along.astype(jnp.bfloat16)
        down = lax.broadcasted_iota(jnp.int32, (lanes, LANES), 0).astype(jnp.float32)
        down = down.astype(jnp.bfloat16)
        one, zero = jnp.bfloat16(1.0), jnp.bfloat16(0.0)
        for h in range(2 * rows):
            flat = jnp.broadcast_to(lane[h:h + 1], (lanes, LANES)).astype(jnp.bfloat16)
            gather_s[k, :, pl.ds(h * LANES, LANES)] = jnp.where(
                down == flat, one, zero
            ).astype(F8)
            tall = jnp.broadcast_to(turned[:, h:h + 1], (LANES, LANES))
            for q in range(lanes // LANES):
                scatter_s[k, pl.ds(h * LANES, LANES), pl.ds(q * LANES, LANES)] = (
                    jnp.where(along + jnp.bfloat16(q * LANES) == tall, one, zero).astype(F8)
                )

    sub_iota = lax.broadcasted_iota(jnp.int32, (SUB, LANES), 0)

    def hot(k, r, e):
        index = index_s[k, pl.ds(2 * r + e, 1), :]
        return sub_iota == (index >> shift)

    def tables(k):
        position, velocity = data(k)[0], data(k)[1]
        for t, ref in ((0, position), (3, velocity)):
            for c in range(3):
                for r in range(SUB):
                    for q in range(lanes // LANES):
                        table_s[k, pl.ds((t + c) * SUB + r, 1), pl.ds(q * LANES, LANES)] = ref[
                            pl.ds(c, 1), pl.ds(r * lanes + q * LANES, LANES)
                        ]
        place = limbs(table_s[k, pl.ds(0, 3 * SUB), :], 3)
        speed = limbs(table_s[k, pl.ds(3 * SUB, 3 * SUB), :], 2)
        inverse = limbs(masses(k), 2)
        return jnp.concatenate(place + speed + inverse, axis=0)

    def ends(k, stacked, r):
        out = dot(stacked, gather_s[k, :, pl.ds(r * WIDE, WIDE)])

        def take(first, count):
            step = 3 * SUB if first < 15 * SUB else SUB
            total = out[first:first + step]
            for t in range(1, count):
                total = total + out[first + t * step:first + (t + 1) * step]
            return total

        place, speed, inverse = take(0, 3), take(9 * SUB, 2), take(15 * SUB, 2)
        pieces = [place[c * SUB:(c + 1) * SUB] for c in range(3)]
        pieces += [speed[c * SUB:(c + 1) * SUB] for c in range(3)] + [inverse]
        found = []
        for e in range(2):
            mask = hot(k, r, e)
            found.append(
                [jnp.where(mask, p[:, e * LANES:(e + 1) * LANES], 0.0) for p in pieces]
            )
        return found

    def start(k, r, at_i, at_j):
        diff = [row_sum(a - b) for a, b in zip(at_i[0:3], at_j[0:3])]
        rate = [row_sum(a - b) for a, b in zip(at_i[3:6], at_j[3:6])]
        size = jnp.sqrt(inner(diff, diff))
        unit = [d / size for d in diff]
        scale = 1.0 / jnp.sqrt(row_sum(at_i[6] + at_j[6]))
        gap = [d + time_step * v for d, v in zip(diff, rate)]
        size_s[k, pl.ds(r, 1), :] = size
        scale_s[k, pl.ds(r, 1), :] = scale
        for c in range(3):
            gap_s[k, c, pl.ds(r, 1), :] = gap[c]
        rhs_s[k, pl.ds(r, 1), :] = scale * (inner(unit, gap) - size)
        where = (k, k if r < bond_rows else (k + 1) % n)
        for e, sign in ((0, 1.0), (1, -1.0)):
            signed = jnp.where(hot(where[e], r, e), sign, 0.0)
            hot_s[where[e], r, e] = signed
            for c in range(3):
                weight_s[where[e], r, e, c] = signed * (scale * unit[c])

    cross = {}

    def prepare(k):
        index_bonds(k)
        index_cross(k)
        one_hots(k)
        stacked = tables(k)
        for r in range(rows):
            at_i, at_j = ends(k, stacked, r)
            if r < bond_rows:
                start(k, r, at_i, at_j)
            else:
                cross[k, r, 0] = at_i
                cross[(k + n - 1) % n, r, 1] = at_j

    prepare(0)
    for copy in copies:
        copy.wait()
    for k in range(1, n):
        prepare(k)
    for k in range(n):
        for r in range(bond_rows, rows):
            start(k, r, cross[k, r, 0], cross[k, r, 1])

    every = [(k, r) for k in range(n) for r in range(rows)]

    def constraint(k, r, e):
        return (k, r) if e == 0 or r < bond_rows else ((k + n - 1) % n, r)

    def scatter(k, x):
        chains = [None, None]
        for r in range(rows):
            columns = []
            for e in range(2):
                value = x[constraint(k, r, e)]
                high = [value * weight_s[k, r, e, c] for c in range(3)]
                low = [rounded(h) - h for h in high]
                columns.append(jnp.concatenate(high + low, axis=0))
            part = dot(
                jnp.concatenate(columns, axis=1), scatter_s[k, pl.ds(r * WIDE, WIDE), :]
            )
            chains[r % 2] = part if chains[r % 2] is None else chains[r % 2] + part
        weight = masses(k)
        pieces = [
            [
                weight * (p[c * SUB:(c + 1) * SUB] - p[(3 + c) * SUB:(4 + c) * SUB])
                for c in range(3)
            ]
            for p in chains
        ]
        return [a + b for a, b in zip(*pieces)]

    def gather(k, field):
        stacked = jnp.concatenate(field + [rounded(f) - f for f in field], axis=0)
        found = []
        for r in range(rows):
            out = dot(stacked, gather_s[k, :, pl.ds(r * WIDE, WIDE)])
            both = out[:3 * SUB] - out[3 * SUB:]
            found.append([
                [both[c * SUB:(c + 1) * SUB, e * LANES:(e + 1) * LANES] for c in range(3)]
                for e in range(2)
            ])
        return found

    def at_constraints(found, function):
        partial = {}
        for k in range(n):
            for r in range(rows):
                for e in range(2):
                    partial[constraint(k, r, e) + (e,)] = function(k, r, e, found[k][r][e])
        return partial

    def apply(rhs, x):
        fields = [scatter(k, x) for k in range(n)]
        found = [gather(k, fields[k]) for k in range(n)]
        parts = at_constraints(
            found,
            lambda k, r, e, f: inner([weight_s[k, r, e, c] for c in range(3)], f),
        )
        return {
            (k, r): rhs[k, r] + x[k, r] - row_sum(parts[k, r, 0] + parts[k, r, 1])
            for k, r in every
        }

    def expand(rhs):
        if n > 2:
            return lax.fori_loop(0, ORDER, lambda _, x: apply(rhs, x), rhs)
        x = rhs
        for _ in range(ORDER):
            x = apply(rhs, x)
        return x

    def load_rhs():
        return {(k, r): rhs_s[k, pl.ds(r, 1), :] for k, r in every}

    for c in range(3):
        total_s[c] = jnp.zeros((SUB, lanes), jnp.float32)

    def one_round(_, carry):
        x = expand(load_rhs())
        fields = [scatter(k, x) for k in range(n)]
        for c in range(3):
            total_s[c] = total_s[c] + fields[0][c]
        found = [gather(k, fields[k]) for k in range(n)]
        parts = at_constraints(
            found, lambda k, r, e, f: [hot_s[k, r, e] * f[c] for c in range(3)]
        )
        for k, r in every:
            gap = []
            for c in range(3):
                moved = row_sum(parts[k, r, 0][c] + parts[k, r, 1][c])
                gap.append(gap_s[k, c, pl.ds(r, 1), :] - moved)
                gap_s[k, c, pl.ds(r, 1), :] = gap[c]
            size = size_s[k, pl.ds(r, 1), :]
            scale = scale_s[k, pl.ds(r, 1), :]
            rhs_s[k, pl.ds(r, 1), :] = scale * (
                size - jnp.sqrt(2.0 * size * size - inner(gap, gap))
            )
        return carry

    if n > 2:
        lax.fori_loop(0, ITER, one_round, 0)
    else:
        for _ in range(ITER):
            one_round(0, 0)
    last = scatter(0, expand(load_rhs()))
    for c in range(3):
        total_s[c] = (total_s[c] + last[c]) / time_step
    for c in range(3):
        for r in range(SUB):
            for q in range(lanes // LANES):
                cols = pl.ds(r * lanes + q * LANES, LANES)
                out_p[pl.ds(c, 1), cols] = (
                    vel[pl.ds(c, 1), cols]
                    - total_s[c, pl.ds(r, 1), pl.ds(q * LANES, LANES)]
                )


def hand_over(p, w, out_p, out_w):
    out_p[...] = p[...]
    out_w[...] = w[...]


def on_device(
    n, protein_pos, protein_vel, inv_mass, bond_atoms, left_atoms, right_atoms, water_pos, water_vel
):
    atoms = protein_pos.shape[1]
    lanes = atoms // SUB
    halo_rows = left_atoms.shape[0] // LANES
    rows = bond_atoms.shape[1] // LANES + halo_rows
    packed = -(-rows // SUB) * SUB
    ends = -(-2 * rows // SUB) * SUB
    others = max(n - 1, 1)
    mass = inv_mass.reshape(atoms // LANES, LANES)
    left = left_atoms.reshape(halo_rows, LANES)
    right = right_atoms.reshape(halo_rows, LANES)
    operands = (protein_pos, protein_vel, mass, bond_atoms, left, right, water_pos, water_vel)
    vmem = pl.BlockSpec(memory_space=pltpu.VMEM)
    results = pl.pallas_call(
        functools.partial(kernel, n, "dom"),
        out_shape=(
            pltpu.VMEM(protein_vel.shape, jnp.float32),
            pltpu.VMEM(water_vel.shape, jnp.float32),
        ),
        in_specs=[pl.BlockSpec(memory_space=pltpu.HBM)] * len(operands),
        out_specs=(vmem, vmem),
        scratch_shapes=[pltpu.VMEM(x.shape, x.dtype) for x in operands] + [
            pltpu.VMEM((others,) + x.shape, x.dtype) for x in operands[:6]
        ] + [
            pltpu.VMEM((n, ends, LANES), jnp.int32),
            pltpu.VMEM((n, 6 * SUB, lanes), jnp.float32),
            pltpu.VMEM((n, rows * WIDE, lanes), F8),
            pltpu.VMEM((n, lanes, rows * WIDE), F8),
            pltpu.VMEM((n, rows, 2, 3, SUB, LANES), jnp.float32),
            pltpu.VMEM((n, rows, 2, SUB, LANES), jnp.float32),
            pltpu.VMEM((n, packed, LANES), jnp.float32),
            pltpu.VMEM((n, packed, LANES), jnp.float32),
            pltpu.VMEM((n, 3, packed, LANES), jnp.float32),
            pltpu.VMEM((n, packed, LANES), jnp.float32),
            pltpu.VMEM((3, SUB, lanes), jnp.float32),
            pltpu.VMEM((2 * water_pos.shape[0], water_pos.shape[1] // LANES, LANES), jnp.float32),
            pltpu.SemaphoreType.DMA((len(operands),)),
            pltpu.SemaphoreType.DMA((others, 6)),
            pltpu.SemaphoreType.DMA((others, 6)),
        ],
        compiler_params=pltpu.CompilerParams(
            collective_id=0, has_side_effects=True, vmem_limit_bytes=60 * 1024 * 1024
        ),
    )(*operands)
    return pl.pallas_call(
        hand_over,
        out_shape=[jax.ShapeDtypeStruct(x.shape, x.dtype) for x in results],
        in_specs=[vmem] * 2,
        out_specs=[vmem] * 2,
        compiler_params=pltpu.CompilerParams(vmem_limit_bytes=8 * 1024 * 1024),
    )(*results)


def solution(mesh):
    in_specs = (
        P(None, ("rep", "dom")),
        P(None, ("rep", "dom")),
        P(("rep", "dom")),
        P(None, ("rep", "dom")),
        P(("rep", "dom")),
        P(("rep", "dom")),
        P(None, ("rep", "dom")),
        P(None, ("rep", "dom")),
    )
    out_specs = (P(None, ("rep", "dom")), P(None, ("rep", "dom")))
    return jax.shard_map(
        functools.partial(on_device, mesh.shape["dom"]),
        mesh=mesh, in_specs=in_specs, out_specs=out_specs, check_vma=False,
    )
```

```python
import functools
import math

import jax
import jax.numpy as jnp
from jax import lax
from jax.experimental import pallas as pl
from jax.experimental.pallas import tpu as pltpu
from jax.sharding import PartitionSpec as P

ORDER = 4
ITER = 2
LANES = 128
SUB = 8
WIDE = 2 * LANES
F8 = jnp.float8_e4m3fn


time_step = 0.002
mass_oxygen = 15.9994
mass_hydrogen = 1.008
oxygen_hydrogen = 0.09572
hydrogen_pair = 0.15139
total_mass = mass_oxygen + 2.0 * mass_hydrogen
half_pair = 0.5 * hydrogen_pair
water_height = math.sqrt(oxygen_hydrogen * oxygen_hydrogen - half_pair * half_pair)
oxygen_reach = 2.0 * mass_hydrogen * water_height / total_mass
hydrogen_reach = water_height - oxygen_reach


def cross_product(left, right):
    return [
        left[1] * right[2] - left[2] * right[1],
        left[2] * right[0] - left[0] * right[2],
        left[0] * right[1] - left[1] * right[0],
    ]


def inner(left, right):
    return left[0] * right[0] + left[1] * right[1] + left[2] * right[2]


def minus(left, right):
    return [a - b for a, b in zip(left, right)]


def settle(before, after):
    old_oxygen, old_first, old_second = (before[0:3], before[3:6], before[6:9])
    new_oxygen, new_first, new_second = (after[0:3], after[3:6], after[6:9])
    center = [
        (mass_oxygen * o + mass_hydrogen * (f + s)) / total_mass
        for o, f, s in zip(new_oxygen, new_first, new_second)
    ]
    old_b = minus(old_first, old_oxygen)
    old_c = minus(old_second, old_oxygen)
    rel_a = minus(new_oxygen, center)
    rel_b = minus(new_first, center)
    rel_c = minus(new_second, center)
    normal = cross_product(old_b, old_c)
    side = cross_product(rel_a, normal)
    upward = cross_product(normal, side)

    def normed(vector):
        size = jnp.sqrt(inner(vector, vector))
        return [a / size for a in vector]

    axis_z = normed(normal)
    axis_x = normed(side)
    axis_y = normed(upward)
    oldb_x = inner(axis_x, old_b)
    oldb_y = inner(axis_y, old_b)
    oldc_x = inner(axis_x, old_c)
    oldc_y = inner(axis_y, old_c)
    newa_z = inner(axis_z, rel_a)
    newb_x = inner(axis_x, rel_b)
    newb_y = inner(axis_y, rel_b)
    newb_z = inner(axis_z, rel_b)
    newc_x = inner(axis_x, rel_c)
    newc_y = inner(axis_y, rel_c)
    newc_z = inner(axis_z, rel_c)
    sin_phi = newa_z / oxygen_reach
    cos_phi = jnp.sqrt(1.0 - sin_phi * sin_phi)
    sin_psi = (newb_z - newc_z) / (2.0 * half_pair * cos_phi)
    cos_psi = jnp.sqrt(1.0 - sin_psi * sin_psi)
    rest_ay = oxygen_reach * cos_phi
    rest_bx = -half_pair * cos_psi
    lowered = -hydrogen_reach * cos_phi
    tilted = half_pair * sin_psi * sin_phi
    rest_by = lowered - tilted
    rest_cy = lowered + tilted
    alpha = rest_bx * (oldb_x - oldc_x) + oldb_y * rest_by + oldc_y * rest_cy
    beta = rest_bx * (oldc_y - oldb_y) + oldb_x * rest_by + oldc_x * rest_cy
    gamma = oldb_x * newb_y - newb_x * oldb_y + oldc_x * newc_y - newc_x * oldc_y
    summed = alpha * alpha + beta * beta
    sin_theta = (alpha * gamma - beta * jnp.sqrt(summed - gamma * gamma)) / summed
    cos_theta = jnp.sqrt(1.0 - sin_theta * sin_theta)
    final_ax = -rest_ay * sin_theta
    final_ay = rest_ay * cos_theta
    final_bx = rest_bx * cos_theta - rest_by * sin_theta
    final_by = rest_bx * sin_theta + rest_by * cos_theta
    final_cx = -rest_bx * cos_theta - rest_cy * sin_theta
    final_cy = -rest_bx * sin_theta + rest_cy * cos_theta

    def placed(x, y, z):
        return [
            center[c] + axis_x[c] * x + axis_y[c] * y + axis_z[c] * z for c in range(3)
        ]

    return (
        placed(final_ax, final_ay, newa_z)
        + placed(final_bx, final_by, newb_z)
        + placed(final_cx, final_cy, newc_z)
    )


def rounded(x):
    return x.astype(jnp.bfloat16).astype(jnp.float32)


def limbs(x, count):
    parts = []
    for _ in range(count - 1):
        part = rounded(x)
        parts.append(part)
        x = x - part
    return parts + [x]


def dot(a, b):
    return lax.dot_general(
        a, b, (((1,), (0,)), ((), ())), preferred_element_type=jnp.float32
    )


def row_sum(x):
    return jnp.sum(x, axis=0, keepdims=True)


def kernel(
    n, axis, *refs
):
    given, refs = refs[:8], refs[8:]
    out_p, out_w = refs[:2]
    pos, vel, mass, bonds, left, right, wpos, wvel = refs[2:10]
    pos_x, vel_x, mass_x, bonds_x, left_x, right_x = refs[10:16]
    (
    index_s, table_s, scatter_s, gather_s, weight_s, hot_s,
    size_s, scale_s, gap_s, rhs_s, tile_s, field_s, total_s, water_s,
    load_sem, send_sem, recv_sem,
    ) = refs[16:]
    atoms = pos.shape[1]
    lanes = atoms // SUB
    shift = lanes.bit_length() - 1
    bond_rows = bonds.shape[1] // LANES
    halo_rows = left.shape[0]
    rows = bond_rows + halo_rows
    pairs = SUB // 2
    groups = [min(1 if k == 0 else 2, bond_rows // pairs) for k in range(n)]
    picked = [g * pairs for g in groups]
    water_rows = wpos.shape[1] // LANES

    own = (pos, vel, mass, bonds, left, right)
    others = (pos_x, vel_x, mass_x, bonds_x, left_x, right_x)
    me = lax.axis_index(axis)
    loads = [
        pltpu.make_async_copy(source, to, load_sem.at[t])
        for t, (source, to) in enumerate(zip(given, own + (wpos, wvel)))
    ]
    for load in loads:
        load.start()
    copies = []
    if n > 1:
        barrier = pltpu.get_barrier_semaphore()
        for k in range(1, n):
            peer = lax.rem(me + k, n)
            pl.semaphore_signal(
                barrier, inc=1, device_id={axis: peer},
                device_id_type=pl.DeviceIdType.MESH,
            )
    for load in loads[:len(own)]:
        load.wait()
    if n > 1:
        pl.semaphore_wait(barrier, n - 1)
        for k in range(1, n):
            peer = lax.rem(me + n - k, n)
            for t in range(len(own)):
                copy = pltpu.make_async_remote_copy(
                    src_ref=own[t],
                    dst_ref=others[t].at[k - 1],
                    send_sem=send_sem.at[k - 1, t],
                    recv_sem=recv_sem.at[k - 1, t],
                    device_id={axis: peer},
                    device_id_type=pl.DeviceIdType.MESH,
                )
                copy.start()
                copies.append(copy)

    for load in loads[len(own):]:
        load.wait()
    components = wpos.shape[0]
    for source, base in ((wpos, 0), (wvel, components)):
        for c in range(components):
            for r in range(water_rows):
                water_s[base + c, pl.ds(r, 1), :] = source[
                    pl.ds(c, 1), pl.ds(r * LANES, LANES)
                ]
    before = [water_s[c] for c in range(components)]
    speed = [water_s[components + c] for c in range(components)]
    after = [b + time_step * v for b, v in zip(before, speed)]
    settled = settle(before, after)
    for c in range(components):
        water_s[c] = speed[c] + (settled[c] - after[c]) / time_step
    for c in range(components):
        for r in range(water_rows):
            out_w[pl.ds(c, 1), pl.ds(r * LANES, LANES)] = water_s[c, pl.ds(r, 1), :]

    def data(k):
        return own if k == 0 else tuple(ref.at[k - 1] for ref in others)

    def masses(k):
        ref = data(k)[2]
        step = lanes // LANES
        return jnp.concatenate(
            [ref[pl.ds(h, SUB, stride=step), :] for h in range(step)], axis=1
        )

    def index_bonds(k):
        ref = data(k)[3]
        for r in range(bond_rows):
            for e in range(2):
                index_s[k, pl.ds(2 * r + e, 1), :] = ref[
                    pl.ds(e, 1), pl.ds(r * LANES, LANES)
                ]

    def index_cross(k):
        for r in range(halo_rows):
            for e, ref in ((0, data(k)[5]), (1, data(k)[4])):
                index_s[k, pl.ds(2 * (bond_rows + r) + e, 1), :] = ref[pl.ds(r, 1), :]

    def one_hots(k):
        lane = (index_s[k] & (lanes - 1)).astype(jnp.float32)
        turned = lane.T.astype(jnp.bfloat16)
        along = lax.broadcasted_iota(jnp.int32, (LANES, LANES), 1).astype(jnp.float32)
        along = along.astype(jnp.bfloat16)
        down = lax.broadcasted_iota(jnp.int32, (lanes, LANES), 0).astype(jnp.float32)
        down = down.astype(jnp.bfloat16)
        one, zero = jnp.bfloat16(1.0), jnp.bfloat16(0.0)
        for h in range(2 * rows):
            flat = jnp.broadcast_to(lane[h:h + 1], (lanes, LANES)).astype(jnp.bfloat16)
            gather_s[k, :, pl.ds(h * LANES, LANES)] = jnp.where(
                down == flat, one, zero
            ).astype(F8)
            tall = jnp.broadcast_to(turned[:, h:h + 1], (LANES, LANES))
            for q in range(lanes // LANES):
                scatter_s[k, pl.ds(h * LANES, LANES), pl.ds(q * LANES, LANES)] = (
                    jnp.where(along + jnp.bfloat16(q * LANES) == tall, one, zero).astype(F8)
                )

    sub_iota = lax.broadcasted_iota(jnp.int32, (SUB, LANES), 0)

    def hot(k, r, e):
        index = index_s[k, pl.ds(2 * r + e, 1), :]
        return sub_iota == (index >> shift)

    def tables(k):
        position, velocity = data(k)[0], data(k)[1]
        for t, ref in ((0, position), (3, velocity)):
            for c in range(3):
                for r in range(SUB):
                    for q in range(lanes // LANES):
                        table_s[k, pl.ds((t + c) * SUB + r, 1), pl.ds(q * LANES, LANES)] = ref[
                            pl.ds(c, 1), pl.ds(r * lanes + q * LANES, LANES)
                        ]
        place = limbs(table_s[k, pl.ds(0, 3 * SUB), :], 3)
        speed = limbs(table_s[k, pl.ds(3 * SUB, 3 * SUB), :], 2)
        inverse = limbs(masses(k), 2)
        return jnp.concatenate(place + speed + inverse, axis=0)

    def ends(k, stacked, r):
        out = dot(stacked, gather_s[k, :, pl.ds(r * WIDE, WIDE)])

        def take(first, count):
            step = 3 * SUB if first < 15 * SUB else SUB
            total = out[first:first + step]
            for t in range(1, count):
                total = total + out[first + t * step:first + (t + 1) * step]
            return total

        place, speed, inverse = take(0, 3), take(9 * SUB, 2), take(15 * SUB, 2)
        pieces = [place[c * SUB:(c + 1) * SUB] for c in range(3)]
        pieces += [speed[c * SUB:(c + 1) * SUB] for c in range(3)] + [inverse]
        found = []
        for e in range(2):
            mask = hot(k, r, e)
            found.append(
                [jnp.where(mask, p[:, e * LANES:(e + 1) * LANES], 0.0) for p in pieces]
            )
        return found

    def start(k, r, at_i, at_j):
        diff = [row_sum(a - b) for a, b in zip(at_i[0:3], at_j[0:3])]
        rate = [row_sum(a - b) for a, b in zip(at_i[3:6], at_j[3:6])]
        size = jnp.sqrt(inner(diff, diff))
        unit = [d / size for d in diff]
        scale = 1.0 / jnp.sqrt(row_sum(at_i[6] + at_j[6]))
        gap = [d + time_step * v for d, v in zip(diff, rate)]
        size_s[k, pl.ds(r, 1), :] = size
        scale_s[k, pl.ds(r, 1), :] = scale
        for c in range(3):
            gap_s[k, c, pl.ds(r, 1), :] = gap[c]
        rhs_s[k, pl.ds(r, 1), :] = scale * (inner(unit, gap) - size)
        where = (k, k if r < bond_rows else (k + 1) % n)
        for e, sign in ((0, 1.0), (1, -1.0)):
            signed = jnp.where(hot(where[e], r, e), sign, 0.0)
            hot_s[where[e], r, e] = signed
            for c in range(3):
                weight = scale * unit[c]
                weight_s[where[e], r, e, c] = signed * weight
                if r < picked[k]:
                    tile_s[k, r // pairs, c, pl.ds(2 * (r % pairs) + e, 1), :] = (
                        sign * weight
                    )

    cross = {}

    def prepare(k):
        index_bonds(k)
        index_cross(k)
        one_hots(k)
        stacked = tables(k)
        for r in range(rows):
            at_i, at_j = ends(k, stacked, r)
            if r < bond_rows:
                start(k, r, at_i, at_j)
            else:
                cross[k, r, 0] = at_i
                cross[(k + n - 1) % n, r, 1] = at_j

    prepare(0)
    for copy in copies:
        copy.wait()
    for k in range(1, n):
        prepare(k)
    for k in range(n):
        for r in range(bond_rows, rows):
            start(k, r, cross[k, r, 0], cross[k, r, 1])

    every = [(k, r) for k in range(n) for r in range(rows)]

    def constraint(k, r, e):
        return (k, r) if e == 0 or r < bond_rows else ((k + n - 1) % n, r)

    def scatter(k, x):
        chains = [None, None]
        for r in range(rows):
            columns = []
            for e in range(2):
                value = x[constraint(k, r, e)]
                high = [value * weight_s[k, r, e, c] for c in range(3)]
                low = [rounded(h) - h for h in high]
                columns.append(jnp.concatenate(high + low, axis=0))
            part = dot(
                jnp.concatenate(columns, axis=1), scatter_s[k, pl.ds(r * WIDE, WIDE), :]
            )
            chains[r % 2] = part if chains[r % 2] is None else chains[r % 2] + part
        weight = masses(k)
        pieces = [
            [
                weight * (p[c * SUB:(c + 1) * SUB] - p[(3 + c) * SUB:(4 + c) * SUB])
                for c in range(3)
            ]
            for p in chains
        ]
        return [a + b for a, b in zip(*pieces)]

    def gather(k, field):
        stacked = jnp.concatenate(field + [rounded(f) - f for f in field], axis=0)
        found = [None] * picked[k]
        for r in range(picked[k], rows):
            out = dot(stacked, gather_s[k, :, pl.ds(r * WIDE, WIDE)])
            both = out[:3 * SUB] - out[3 * SUB:]
            found.append([
                [both[c * SUB:(c + 1) * SUB, e * LANES:(e + 1) * LANES] for c in range(3)]
                for e in range(2)
            ])
        return found

    def pick(k, g):
        index = index_s[k, pl.ds(g * SUB, SUB), :]
        lane, block = index & (LANES - 1), index >> (LANES.bit_length() - 1)
        taken = [None] * 3
        per_row = lanes // LANES
        for s in range(SUB):
            for q in range(per_row):
                hit = block == s * per_row + q
                for c in range(3):
                    source = jnp.broadcast_to(
                        field_s[k, c, pl.ds(s, 1), pl.ds(q * LANES, LANES)], (SUB, LANES)
                    )
                    got = jnp.take_along_axis(
                        source, lane, axis=1, mode="promise_in_bounds"
                    )
                    old = taken[c]
                    taken[c] = got if old is None else jnp.where(hit, got, old)
        return taken

    def picks(fields):
        for k in range(n):
            for c in range(3):
                field_s[k, c] = fields[k][c]
        return [[pick(k, g) for g in range(groups[k])] for k in range(n)]

    def at_even(x, q):
        return jnp.broadcast_to(x[2 * q:2 * q + 1], (SUB, LANES))

    def at_constraints(found, function):
        partial = {}
        for k in range(n):
            for r in range(picked[k], rows):
                for e in range(2):
                    partial[constraint(k, r, e) + (e,)] = function(k, r, e, found[k][r][e])
        return partial

    def apply(rhs, x):
        fields = [scatter(k, x) for k in range(n)]
        taken = picks(fields)
        found = [gather(k, fields[k]) for k in range(n)]
        parts = at_constraints(
            found,
            lambda k, r, e, f: inner([weight_s[k, r, e, c] for c in range(3)], f),
        )
        near = [
            [inner([tile_s[k, g, c] for c in range(3)], taken[k][g]) for g in range(groups[k])]
            for k in range(n)
        ]
        near = [[t + pltpu.roll(t, SUB - 1, 0) for t in some] for some in near]

        def change(k, r):
            if r < picked[k]:
                return at_even(near[k][r // pairs], r % pairs)
            return row_sum(parts[k, r, 0] + parts[k, r, 1])

        return {(k, r): rhs[k, r] + x[k, r] - change(k, r) for k, r in every}

    def expand(rhs):
        if n > 2:
            return lax.fori_loop(0, ORDER, lambda _, x: apply(rhs, x), rhs)
        x = rhs
        for _ in range(ORDER):
            x = apply(rhs, x)
        return x

    def load_rhs():
        return {
            (k, r): jnp.broadcast_to(rhs_s[k, pl.ds(r, 1), :], (SUB, LANES))
            for k, r in every
        }

    for c in range(3):
        total_s[c] = jnp.zeros((SUB, lanes), jnp.float32)

    def one_round(_, carry):
        x = expand(load_rhs())
        fields = [scatter(k, x) for k in range(n)]
        for c in range(3):
            total_s[c] = total_s[c] + fields[0][c]
        taken = picks(fields)
        found = [gather(k, fields[k]) for k in range(n)]
        parts = at_constraints(
            found, lambda k, r, e, f: [hot_s[k, r, e] * f[c] for c in range(3)]
        )
        near = [
            [[t - pltpu.roll(t, SUB - 1, 0) for t in some] for some in taken[k]]
            for k in range(n)
        ]
        for k, r in every:
            gap = []
            for c in range(3):
                if r < picked[k]:
                    q = 2 * (r % pairs)
                    moved = near[k][r // pairs][c][q:q + 1]
                else:
                    moved = row_sum(parts[k, r, 0][c] + parts[k, r, 1][c])
                gap.append(gap_s[k, c, pl.ds(r, 1), :] - moved)
                gap_s[k, c, pl.ds(r, 1), :] = gap[c]
            size = size_s[k, pl.ds(r, 1), :]
            scale = scale_s[k, pl.ds(r, 1), :]
            rhs_s[k, pl.ds(r, 1), :] = scale * (
                size - jnp.sqrt(2.0 * size * size - inner(gap, gap))
            )
        return carry

    if n > 2:
        lax.fori_loop(0, ITER, one_round, 0)
    else:
        for _ in range(ITER):
            one_round(0, 0)
    last = scatter(0, expand(load_rhs()))
    for c in range(3):
        total_s[c] = (total_s[c] + last[c]) / time_step
    for c in range(3):
        for r in range(SUB):
            for q in range(lanes // LANES):
                cols = pl.ds(r * lanes + q * LANES, LANES)
                out_p[pl.ds(c, 1), cols] = (
                    vel[pl.ds(c, 1), cols]
                    - total_s[c, pl.ds(r, 1), pl.ds(q * LANES, LANES)]
                )


def hand_over(p, w, out_p, out_w):
    out_p[...] = p[...]
    out_w[...] = w[...]


def on_device(
    n, protein_pos, protein_vel, inv_mass, bond_atoms, left_atoms, right_atoms, water_pos, water_vel
):
    atoms = protein_pos.shape[1]
    lanes = atoms // SUB
    halo_rows = left_atoms.shape[0] // LANES
    rows = bond_atoms.shape[1] // LANES + halo_rows
    packed = -(-rows // SUB) * SUB
    ends = -(-2 * rows // SUB) * SUB
    others = max(n - 1, 1)
    mass = inv_mass.reshape(atoms // LANES, LANES)
    left = left_atoms.reshape(halo_rows, LANES)
    right = right_atoms.reshape(halo_rows, LANES)
    operands = (protein_pos, protein_vel, mass, bond_atoms, left, right, water_pos, water_vel)
    vmem = pl.BlockSpec(memory_space=pltpu.VMEM)
    results = pl.pallas_call(
        functools.partial(kernel, n, "dom"),
        out_shape=(
            pltpu.VMEM(protein_vel.shape, jnp.float32),
            pltpu.VMEM(water_vel.shape, jnp.float32),
        ),
        in_specs=[pl.BlockSpec(memory_space=pltpu.HBM)] * len(operands),
        out_specs=(vmem, vmem),
        scratch_shapes=[pltpu.VMEM(x.shape, x.dtype) for x in operands] + [
            pltpu.VMEM((others,) + x.shape, x.dtype) for x in operands[:6]
        ] + [
            pltpu.VMEM((n, ends, LANES), jnp.int32),
            pltpu.VMEM((n, 6 * SUB, lanes), jnp.float32),
            pltpu.VMEM((n, rows * WIDE, lanes), F8),
            pltpu.VMEM((n, lanes, rows * WIDE), F8),
            pltpu.VMEM((n, rows, 2, 3, SUB, LANES), jnp.float32),
            pltpu.VMEM((n, rows, 2, SUB, LANES), jnp.float32),
            pltpu.VMEM((n, packed, LANES), jnp.float32),
            pltpu.VMEM((n, packed, LANES), jnp.float32),
            pltpu.VMEM((n, 3, packed, LANES), jnp.float32),
            pltpu.VMEM((n, packed, LANES), jnp.float32),
            pltpu.VMEM((n, rows, 3, SUB, LANES), jnp.float32),
            pltpu.VMEM((n, 3, SUB, lanes), jnp.float32),
            pltpu.VMEM((3, SUB, lanes), jnp.float32),
            pltpu.VMEM((2 * water_pos.shape[0], water_pos.shape[1] // LANES, LANES), jnp.float32),
            pltpu.SemaphoreType.DMA((len(operands),)),
            pltpu.SemaphoreType.DMA((others, 6)),
            pltpu.SemaphoreType.DMA((others, 6)),
        ],
        compiler_params=pltpu.CompilerParams(
            collective_id=0, has_side_effects=True, vmem_limit_bytes=60 * 1024 * 1024
        ),
    )(*operands)
    return pl.pallas_call(
        hand_over,
        out_shape=[jax.ShapeDtypeStruct(x.shape, x.dtype) for x in results],
        in_specs=[vmem] * 2,
        out_specs=[vmem] * 2,
        compiler_params=pltpu.CompilerParams(vmem_limit_bytes=8 * 1024 * 1024),
    )(*results)


def solution(mesh):
    in_specs = (
        P(None, ("rep", "dom")),
        P(None, ("rep", "dom")),
        P(("rep", "dom")),
        P(None, ("rep", "dom")),
        P(("rep", "dom")),
        P(("rep", "dom")),
        P(None, ("rep", "dom")),
        P(None, ("rep", "dom")),
    )
    out_specs = (P(None, ("rep", "dom")), P(None, ("rep", "dom")))
    return jax.shard_map(
        functools.partial(on_device, mesh.shape["dom"]),
        mesh=mesh, in_specs=in_specs, out_specs=out_specs, check_vma=False,
    )
```

```python
import functools
import math

import jax
import jax.numpy as jnp
from jax import lax
from jax.experimental import pallas as pl
from jax.experimental.pallas import tpu as pltpu
from jax.sharding import PartitionSpec as P

ORDER = 4
ITER = 2
LANES = 128
SUB = 8
WIDE = 2 * LANES
F8 = jnp.float8_e4m3fn


time_step = 0.002
mass_oxygen = 15.9994
mass_hydrogen = 1.008
oxygen_hydrogen = 0.09572
hydrogen_pair = 0.15139
total_mass = mass_oxygen + 2.0 * mass_hydrogen
half_pair = 0.5 * hydrogen_pair
water_height = math.sqrt(oxygen_hydrogen * oxygen_hydrogen - half_pair * half_pair)
oxygen_reach = 2.0 * mass_hydrogen * water_height / total_mass
hydrogen_reach = water_height - oxygen_reach


def cross_product(left, right):
    return [
        left[1] * right[2] - left[2] * right[1],
        left[2] * right[0] - left[0] * right[2],
        left[0] * right[1] - left[1] * right[0],
    ]


def inner(left, right):
    return left[0] * right[0] + left[1] * right[1] + left[2] * right[2]


def minus(left, right):
    return [a - b for a, b in zip(left, right)]


def settle(before, after):
    old_oxygen, old_first, old_second = (before[0:3], before[3:6], before[6:9])
    new_oxygen, new_first, new_second = (after[0:3], after[3:6], after[6:9])
    center = [
        (mass_oxygen * o + mass_hydrogen * (f + s)) / total_mass
        for o, f, s in zip(new_oxygen, new_first, new_second)
    ]
    old_b = minus(old_first, old_oxygen)
    old_c = minus(old_second, old_oxygen)
    rel_a = minus(new_oxygen, center)
    rel_b = minus(new_first, center)
    rel_c = minus(new_second, center)
    normal = cross_product(old_b, old_c)
    side = cross_product(rel_a, normal)
    upward = cross_product(normal, side)

    def normed(vector):
        size = jnp.sqrt(inner(vector, vector))
        return [a / size for a in vector]

    axis_z = normed(normal)
    axis_x = normed(side)
    axis_y = normed(upward)
    oldb_x = inner(axis_x, old_b)
    oldb_y = inner(axis_y, old_b)
    oldc_x = inner(axis_x, old_c)
    oldc_y = inner(axis_y, old_c)
    newa_z = inner(axis_z, rel_a)
    newb_x = inner(axis_x, rel_b)
    newb_y = inner(axis_y, rel_b)
    newb_z = inner(axis_z, rel_b)
    newc_x = inner(axis_x, rel_c)
    newc_y = inner(axis_y, rel_c)
    newc_z = inner(axis_z, rel_c)
    sin_phi = newa_z / oxygen_reach
    cos_phi = jnp.sqrt(1.0 - sin_phi * sin_phi)
    sin_psi = (newb_z - newc_z) / (2.0 * half_pair * cos_phi)
    cos_psi = jnp.sqrt(1.0 - sin_psi * sin_psi)
    rest_ay = oxygen_reach * cos_phi
    rest_bx = -half_pair * cos_psi
    lowered = -hydrogen_reach * cos_phi
    tilted = half_pair * sin_psi * sin_phi
    rest_by = lowered - tilted
    rest_cy = lowered + tilted
    alpha = rest_bx * (oldb_x - oldc_x) + oldb_y * rest_by + oldc_y * rest_cy
    beta = rest_bx * (oldc_y - oldb_y) + oldb_x * rest_by + oldc_x * rest_cy
    gamma = oldb_x * newb_y - newb_x * oldb_y + oldc_x * newc_y - newc_x * oldc_y
    summed = alpha * alpha + beta * beta
    sin_theta = (alpha * gamma - beta * jnp.sqrt(summed - gamma * gamma)) / summed
    cos_theta = jnp.sqrt(1.0 - sin_theta * sin_theta)
    final_ax = -rest_ay * sin_theta
    final_ay = rest_ay * cos_theta
    final_bx = rest_bx * cos_theta - rest_by * sin_theta
    final_by = rest_bx * sin_theta + rest_by * cos_theta
    final_cx = -rest_bx * cos_theta - rest_cy * sin_theta
    final_cy = -rest_bx * sin_theta + rest_cy * cos_theta

    def placed(x, y, z):
        return [
            center[c] + axis_x[c] * x + axis_y[c] * y + axis_z[c] * z for c in range(3)
        ]

    return (
        placed(final_ax, final_ay, newa_z)
        + placed(final_bx, final_by, newb_z)
        + placed(final_cx, final_cy, newc_z)
    )


def rounded(x):
    return x.astype(jnp.bfloat16).astype(jnp.float32)


def limbs(x, count):
    parts = []
    for _ in range(count - 1):
        part = rounded(x)
        parts.append(part)
        x = x - part
    return parts + [x]


def dot(a, b):
    return lax.dot_general(
        a, b, (((1,), (0,)), ((), ())), preferred_element_type=jnp.float32
    )


def row_sum(x):
    return jnp.sum(x, axis=0, keepdims=True)


def kernel(
    n, axis, *refs
):
    given, refs = refs[:8], refs[8:]
    out_p, out_w = refs[:2]
    pos, vel, mass, bonds, left, right, wpos, wvel = refs[2:10]
    pos_x, vel_x, mass_x, bonds_x, left_x, right_x = refs[10:16]
    (
    index_s, table_s, scatter_s, gather_s, weight_s, hot_s,
    raw_s, size_s, scale_s, gap_s, rhs_s, tile_s, field_s, total_s, water_s,
    load_sem, send_sem, recv_sem,
    ) = refs[16:]
    atoms = pos.shape[1]
    lanes = atoms // SUB
    shift = lanes.bit_length() - 1
    bond_rows = bonds.shape[1] // LANES
    halo_rows = left.shape[0]
    rows = bond_rows + halo_rows
    pairs = SUB // 2
    groups = [min(1 if k == 0 else 2, bond_rows // pairs) for k in range(n)]
    picked = [g * pairs for g in groups]
    water_rows = wpos.shape[1] // LANES

    own = (pos, vel, mass, bonds, left, right)
    others = (pos_x, vel_x, mass_x, bonds_x, left_x, right_x)
    me = lax.axis_index(axis)
    loads = [
        pltpu.make_async_copy(source, to, load_sem.at[t])
        for t, (source, to) in enumerate(zip(given, own + (wpos, wvel)))
    ]
    for load in loads:
        load.start()
    copies = []
    if n > 1:
        barrier = pltpu.get_barrier_semaphore()
        for k in range(1, n):
            peer = lax.rem(me + k, n)
            pl.semaphore_signal(
                barrier, inc=1, device_id={axis: peer},
                device_id_type=pl.DeviceIdType.MESH,
            )
    for load in loads[:len(own)]:
        load.wait()
    if n > 1:
        pl.semaphore_wait(barrier, n - 1)
        for k in range(1, n):
            peer = lax.rem(me + n - k, n)
            for t in range(len(own)):
                copy = pltpu.make_async_remote_copy(
                    src_ref=own[t],
                    dst_ref=others[t].at[k - 1],
                    send_sem=send_sem.at[k - 1, t],
                    recv_sem=recv_sem.at[k - 1, t],
                    device_id={axis: peer},
                    device_id_type=pl.DeviceIdType.MESH,
                )
                copy.start()
                copies.append(copy)

    for load in loads[len(own):]:
        load.wait()
    components = wpos.shape[0]
    for source, base in ((wpos, 0), (wvel, components)):
        for c in range(components):
            for r in range(water_rows):
                water_s[base + c, pl.ds(r, 1), :] = source[
                    pl.ds(c, 1), pl.ds(r * LANES, LANES)
                ]
    before = [water_s[c] for c in range(components)]
    speed = [water_s[components + c] for c in range(components)]
    after = [b + time_step * v for b, v in zip(before, speed)]
    settled = settle(before, after)
    for c in range(components):
        water_s[c] = speed[c] + (settled[c] - after[c]) / time_step
    for c in range(components):
        for r in range(water_rows):
            out_w[pl.ds(c, 1), pl.ds(r * LANES, LANES)] = water_s[c, pl.ds(r, 1), :]

    def data(k):
        return own if k == 0 else tuple(ref.at[k - 1] for ref in others)

    def masses(k):
        ref = data(k)[2]
        step = lanes // LANES
        return jnp.concatenate(
            [ref[pl.ds(h, SUB, stride=step), :] for h in range(step)], axis=1
        )

    def index_bonds(k):
        ref = data(k)[3]
        for r in range(bond_rows):
            for e in range(2):
                index_s[k, pl.ds(2 * r + e, 1), :] = ref[
                    pl.ds(e, 1), pl.ds(r * LANES, LANES)
                ]

    def index_cross(k):
        for r in range(halo_rows):
            for e, ref in ((0, data(k)[5]), (1, data(k)[4])):
                index_s[k, pl.ds(2 * (bond_rows + r) + e, 1), :] = ref[pl.ds(r, 1), :]

    def one_hots(k):
        lane = (index_s[k] & (lanes - 1)).astype(jnp.float32)
        turned = lane.T.astype(jnp.bfloat16)
        along = lax.broadcasted_iota(jnp.int32, (LANES, LANES), 1).astype(jnp.float32)
        along = along.astype(jnp.bfloat16)
        down = lax.broadcasted_iota(jnp.int32, (lanes, LANES), 0).astype(jnp.float32)
        down = down.astype(jnp.bfloat16)
        one, zero = jnp.bfloat16(1.0), jnp.bfloat16(0.0)
        for h in range(2 * rows):
            flat = jnp.broadcast_to(lane[h:h + 1], (lanes, LANES)).astype(jnp.bfloat16)
            gather_s[k, :, pl.ds(h * LANES, LANES)] = jnp.where(
                down == flat, one, zero
            ).astype(F8)
            tall = jnp.broadcast_to(turned[:, h:h + 1], (LANES, LANES))
            for q in range(lanes // LANES):
                scatter_s[k, pl.ds(h * LANES, LANES), pl.ds(q * LANES, LANES)] = (
                    jnp.where(along + jnp.bfloat16(q * LANES) == tall, one, zero).astype(F8)
                )

    sub_iota = lax.broadcasted_iota(jnp.int32, (SUB, LANES), 0)

    def hot(k, r, e):
        index = index_s[k, pl.ds(2 * r + e, 1), :]
        return sub_iota == (index >> shift)

    def tables(k):
        position, velocity = data(k)[0], data(k)[1]
        for t, ref in ((0, position), (3, velocity)):
            for c in range(3):
                for r in range(SUB):
                    for q in range(lanes // LANES):
                        table_s[k, pl.ds((t + c) * SUB + r, 1), pl.ds(q * LANES, LANES)] = ref[
                            pl.ds(c, 1), pl.ds(r * lanes + q * LANES, LANES)
                        ]
        place = limbs(table_s[k, pl.ds(0, 3 * SUB), :], 3)
        speed = limbs(table_s[k, pl.ds(3 * SUB, 3 * SUB), :], 2)
        inverse = limbs(masses(k), 2)
        return jnp.concatenate(place + speed + inverse, axis=0)

    def ends(k, stacked, r):
        out = dot(stacked, gather_s[k, :, pl.ds(r * WIDE, WIDE)])

        def take(first, count):
            step = 3 * SUB if first < 15 * SUB else SUB
            total = out[first:first + step]
            for t in range(1, count):
                total = total + out[first + t * step:first + (t + 1) * step]
            return total

        place, speed, inverse = take(0, 3), take(9 * SUB, 2), take(15 * SUB, 2)
        pieces = [place[c * SUB:(c + 1) * SUB] for c in range(3)]
        pieces += [speed[c * SUB:(c + 1) * SUB] for c in range(3)] + [inverse]
        found = []
        for e in range(2):
            mask = hot(k, r, e)
            found.append(
                [jnp.where(mask, p[:, e * LANES:(e + 1) * LANES], 0.0) for p in pieces]
            )
        return found

    def collect(k, r, at_i, at_j):
        for t in range(6):
            raw_s[k, t, pl.ds(r, 1), :] = row_sum(at_i[t] - at_j[t])
        raw_s[k, 6, pl.ds(r, 1), :] = row_sum(at_i[6] + at_j[6])

    def start(k, first, count):
        span = pl.ds(first, count)
        shape = (count, LANES)
        valid = lax.broadcasted_iota(jnp.int32, shape, 0) < rows - first
        diff = [raw_s[k, c, span, :] for c in range(3)]
        size = jnp.where(valid, jnp.sqrt(inner(diff, diff)), 1.0)
        unit = [d / size for d in diff]
        scale = jnp.where(valid, 1.0 / jnp.sqrt(raw_s[k, 6, span, :]), 0.0)
        gap = [d + time_step * raw_s[k, 3 + c, span, :] for c, d in enumerate(diff)]
        size_s[k, span, :] = size
        scale_s[k, span, :] = scale
        for c in range(3):
            gap_s[k, c, span, :] = gap[c]
            raw_s[k, c, span, :] = scale * unit[c]
        rhs_s[k, span, :] = scale * (inner(unit, gap) - size)
        for r in range(first, min(first + count, rows)):
            weigh(k, r)

    def weigh(k, r):
        where = (k, k if r < bond_rows else (k + 1) % n)
        weight = [raw_s[k, c, pl.ds(r, 1), :] for c in range(3)]
        for e, sign in ((0, 1.0), (1, -1.0)):
            signed = jnp.where(hot(where[e], r, e), sign, 0.0)
            hot_s[where[e], r, e] = signed
            for c in range(3):
                weight_s[where[e], r, e, c] = signed * weight[c]
                if r < picked[k]:
                    tile_s[k, r // pairs, c, pl.ds(2 * (r % pairs) + e, 1), :] = (
                        sign * weight[c]
                    )

    cross = {}

    def prepare(k):
        index_bonds(k)
        index_cross(k)
        one_hots(k)
        stacked = tables(k)
        for r in range(rows):
            at_i, at_j = ends(k, stacked, r)
            if r < bond_rows:
                collect(k, r, at_i, at_j)
            else:
                cross[k, r, 0] = at_i
                cross[(k + n - 1) % n, r, 1] = at_j

    prepare(0)
    whole = bond_rows // SUB * SUB
    if whole:
        start(0, 0, whole)
    for copy in copies:
        copy.wait()
    for k in range(1, n):
        prepare(k)
    for k in range(n):
        for r in range(bond_rows, rows):
            collect(k, r, cross[k, r, 0], cross[k, r, 1])
    for k in range(n):
        first = whole if k == 0 else 0
        start(k, first, size_s.shape[1] - first)

    every = [(k, r) for k in range(n) for r in range(rows)]

    def constraint(k, r, e):
        return (k, r) if e == 0 or r < bond_rows else ((k + n - 1) % n, r)

    def scatter(k, x):
        chains = [None, None]
        for r in range(rows):
            columns = []
            for e in range(2):
                value = x[constraint(k, r, e)]
                high = [value * weight_s[k, r, e, c] for c in range(3)]
                low = [rounded(h) - h for h in high]
                columns.append(jnp.concatenate(high + low, axis=0))
            part = dot(
                jnp.concatenate(columns, axis=1), scatter_s[k, pl.ds(r * WIDE, WIDE), :]
            )
            lot = (r + k) % 2
            chains[lot] = part if chains[lot] is None else chains[lot] + part
        weight = masses(k)
        pieces = [
            [
                weight * (p[c * SUB:(c + 1) * SUB] - p[(3 + c) * SUB:(4 + c) * SUB])
                for c in range(3)
            ]
            for p in chains
        ]
        return [a + b for a, b in zip(*pieces)]

    def gather(k, field):
        stacked = jnp.concatenate(field + [rounded(f) - f for f in field], axis=0)
        found = [None] * rows
        for r in list(range(bond_rows, rows)) + list(range(picked[k], bond_rows)):
            out = dot(stacked, gather_s[k, :, pl.ds(r * WIDE, WIDE)])
            both = out[:3 * SUB] - out[3 * SUB:]
            found[r] = [
                [both[c * SUB:(c + 1) * SUB, e * LANES:(e + 1) * LANES] for c in range(3)]
                for e in range(2)
            ]
        return found

    def pick(k, g):
        index = index_s[k, pl.ds(g * SUB, SUB), :]
        lane, block = index & (LANES - 1), index >> (LANES.bit_length() - 1)
        taken = [None] * 3
        per_row = lanes // LANES
        for s in range(SUB):
            for q in range(per_row):
                hit = block == s * per_row + q
                for c in range(3):
                    source = jnp.broadcast_to(
                        field_s[k, c, pl.ds(s, 1), pl.ds(q * LANES, LANES)], (SUB, LANES)
                    )
                    got = jnp.take_along_axis(
                        source, lane, axis=1, mode="promise_in_bounds"
                    )
                    old = taken[c]
                    taken[c] = got if old is None else jnp.where(hit, got, old)
        return taken

    def picks(fields):
        for k in range(n):
            for c in range(3):
                field_s[k, c] = fields[k][c]
        return [[pick(k, g) for g in range(groups[k])] for k in range(n)]

    def at_even(x, q):
        return jnp.broadcast_to(x[2 * q:2 * q + 1], (SUB, LANES))

    def at_constraints(found, function):
        partial = {}
        for k in range(n):
            for r in range(picked[k], rows):
                for e in range(2):
                    partial[constraint(k, r, e) + (e,)] = function(k, r, e, found[k][r][e])
        return partial

    def apply(rhs, x):
        fields = [scatter(k, x) for k in range(n)]
        taken = picks(fields)
        found = [gather(k, fields[k]) for k in range(n)]
        parts = at_constraints(
            found,
            lambda k, r, e, f: inner([weight_s[k, r, e, c] for c in range(3)], f),
        )
        near = [
            [inner([tile_s[k, g, c] for c in range(3)], taken[k][g]) for g in range(groups[k])]
            for k in range(n)
        ]
        near = [[t + pltpu.roll(t, SUB - 1, 0) for t in some] for some in near]

        def change(k, r):
            if r < picked[k]:
                return at_even(near[k][r // pairs], r % pairs)
            return row_sum(parts[k, r, 0] + parts[k, r, 1])

        return {(k, r): rhs[k, r] + x[k, r] - change(k, r) for k, r in every}

    def expand(rhs):
        if n > 2:
            return lax.fori_loop(0, ORDER, lambda _, x: apply(rhs, x), rhs)
        x = rhs
        for _ in range(ORDER):
            x = apply(rhs, x)
        return x

    def load_rhs():
        return {
            (k, r): jnp.broadcast_to(rhs_s[k, pl.ds(r, 1), :], (SUB, LANES))
            for k, r in every
        }

    for c in range(3):
        total_s[c] = jnp.zeros((SUB, lanes), jnp.float32)

    def one_round(_, carry):
        x = expand(load_rhs())
        fields = [scatter(k, x) for k in range(n)]
        for c in range(3):
            total_s[c] = total_s[c] + fields[0][c]
        taken = picks(fields)
        found = [gather(k, fields[k]) for k in range(n)]
        parts = at_constraints(
            found, lambda k, r, e, f: [hot_s[k, r, e] * f[c] for c in range(3)]
        )
        near = [
            [[t - pltpu.roll(t, SUB - 1, 0) for t in some] for some in taken[k]]
            for k in range(n)
        ]
        for k, r in every:
            gap = []
            for c in range(3):
                if r < picked[k]:
                    q = 2 * (r % pairs)
                    moved = near[k][r // pairs][c][q:q + 1]
                else:
                    moved = row_sum(parts[k, r, 0][c] + parts[k, r, 1][c])
                gap.append(gap_s[k, c, pl.ds(r, 1), :] - moved)
                gap_s[k, c, pl.ds(r, 1), :] = gap[c]
            size = size_s[k, pl.ds(r, 1), :]
            scale = scale_s[k, pl.ds(r, 1), :]
            rhs_s[k, pl.ds(r, 1), :] = scale * (
                size - jnp.sqrt(2.0 * size * size - inner(gap, gap))
            )
        return carry

    if n > 2:
        lax.fori_loop(0, ITER, one_round, 0)
    else:
        for _ in range(ITER):
            one_round(0, 0)
    last = scatter(0, expand(load_rhs()))
    for c in range(3):
        total_s[c] = (total_s[c] + last[c]) / time_step
    for c in range(3):
        for r in range(SUB):
            for q in range(lanes // LANES):
                cols = pl.ds(r * lanes + q * LANES, LANES)
                out_p[pl.ds(c, 1), cols] = (
                    vel[pl.ds(c, 1), cols]
                    - total_s[c, pl.ds(r, 1), pl.ds(q * LANES, LANES)]
                )


def hand_over(p, w, out_p, out_w):
    out_p[...] = p[...]
    out_w[...] = w[...]


def on_device(
    n, protein_pos, protein_vel, inv_mass, bond_atoms, left_atoms, right_atoms, water_pos, water_vel
):
    atoms = protein_pos.shape[1]
    lanes = atoms // SUB
    halo_rows = left_atoms.shape[0] // LANES
    rows = bond_atoms.shape[1] // LANES + halo_rows
    packed = -(-rows // SUB) * SUB
    ends = -(-2 * rows // SUB) * SUB
    others = max(n - 1, 1)
    mass = inv_mass.reshape(atoms // LANES, LANES)
    left = left_atoms.reshape(halo_rows, LANES)
    right = right_atoms.reshape(halo_rows, LANES)
    operands = (protein_pos, protein_vel, mass, bond_atoms, left, right, water_pos, water_vel)
    vmem = pl.BlockSpec(memory_space=pltpu.VMEM)
    results = pl.pallas_call(
        functools.partial(kernel, n, "dom"),
        out_shape=(
            pltpu.VMEM(protein_vel.shape, jnp.float32),
            pltpu.VMEM(water_vel.shape, jnp.float32),
        ),
        in_specs=[pl.BlockSpec(memory_space=pltpu.HBM)] * len(operands),
        out_specs=(vmem, vmem),
        scratch_shapes=[pltpu.VMEM(x.shape, x.dtype) for x in operands] + [
            pltpu.VMEM((others,) + x.shape, x.dtype) for x in operands[:6]
        ] + [
            pltpu.VMEM((n, ends, LANES), jnp.int32),
            pltpu.VMEM((n, 6 * SUB, lanes), jnp.float32),
            pltpu.VMEM((n, rows * WIDE, lanes), F8),
            pltpu.VMEM((n, lanes, rows * WIDE), F8),
            pltpu.VMEM((n, rows, 2, 3, SUB, LANES), jnp.float32),
            pltpu.VMEM((n, rows, 2, SUB, LANES), jnp.float32),
            pltpu.VMEM((n, 7, packed, LANES), jnp.float32),
            pltpu.VMEM((n, packed, LANES), jnp.float32),
            pltpu.VMEM((n, packed, LANES), jnp.float32),
            pltpu.VMEM((n, 3, packed, LANES), jnp.float32),
            pltpu.VMEM((n, packed, LANES), jnp.float32),
            pltpu.VMEM((n, rows, 3, SUB, LANES), jnp.float32),
            pltpu.VMEM((n, 3, SUB, lanes), jnp.float32),
            pltpu.VMEM((3, SUB, lanes), jnp.float32),
            pltpu.VMEM((2 * water_pos.shape[0], water_pos.shape[1] // LANES, LANES), jnp.float32),
            pltpu.SemaphoreType.DMA((len(operands),)),
            pltpu.SemaphoreType.DMA((others, 6)),
            pltpu.SemaphoreType.DMA((others, 6)),
        ],
        compiler_params=pltpu.CompilerParams(
            collective_id=0, has_side_effects=True, vmem_limit_bytes=60 * 1024 * 1024
        ),
    )(*operands)
    return pl.pallas_call(
        hand_over,
        out_shape=[jax.ShapeDtypeStruct(x.shape, x.dtype) for x in results],
        in_specs=[vmem] * 2,
        out_specs=[vmem] * 2,
        compiler_params=pltpu.CompilerParams(vmem_limit_bytes=8 * 1024 * 1024),
    )(*results)


def solution(mesh):
    in_specs = (
        P(None, ("rep", "dom")),
        P(None, ("rep", "dom")),
        P(("rep", "dom")),
        P(None, ("rep", "dom")),
        P(("rep", "dom")),
        P(("rep", "dom")),
        P(None, ("rep", "dom")),
        P(None, ("rep", "dom")),
    )
    out_specs = (P(None, ("rep", "dom")), P(None, ("rep", "dom")))
    return jax.shard_map(
        functools.partial(on_device, mesh.shape["dom"]),
        mesh=mesh, in_specs=in_specs, out_specs=out_specs, check_vma=False,
    )
```
